32 devices in a mesh: gx: 4 (over y, x), gy: 4 (over z), gz: 2 (over core).
Axes of the slice: x: 2, y: 2, z: 4, core: 2. Of those that a mesh axis runs over, the one named last changes fastest.
Arguments:
- layer_east: float32 [16, 512, 512], P('gz', 'gy', 'gx'), may hold values from -6 to 6
- layer_north: float32 [16, 512, 512], P('gz', 'gy', 'gx'), may hold values from -6 to 6
- layer_press: float32 [16, 512, 512], P('gz', 'gy', 'gx'), may hold values from -6 to 6
- surface: float32 [512, 512], P('gy', 'gx'), may hold values from -3 to 3
- land_sea: int32 [512, 512], P('gy', 'gx'), may hold values 0 or 1
- bottom_level: int32 [512, 512], P('gy', 'gx'), may hold values from 12 to 16
- coriolis: float32 [512, 512], P('gy', 'gx'), may hold values from -1 to 1
- level_thick: float32 [16], P('gz'), may hold values from 0.25 to 0.3
Outputs:
- surface_next: float32 [512, 512], P('gy', 'gx')
- east_next: float32 [16, 512, 512], P('gz', 'gy', 'gx')
- north_next: float32 [16, 512, 512], P('gz', 'gy', 'gx')
The draws below stay inside these ranges and needn't reach their ends.
All inputs are finite; a program needn't handle non-finite values. No bound on the sum of `land_sea` on one device may be relied on, other than what follows from the above.
Results may differ from the reference program's by a relative error of at most 0.00002.
Values sent between devices are 32-bit elements; how exact they have to be, the bound alone decides.
No kernel may reach another device: no remote copies, remote signals or barrier semaphores. Data moves between devices by JAX's collectives and lax.ppermute only.
A program may use at most 64 MiB of HBM per device.

```python
import math
import jax
import jax.numpy as jnp

SUBSTEPS = 4
NX = 512
NY = 512
K = 16


def plant(result, rng, low, top_value):
    spot = [jax.random.randint(jax.random.fold_in(rng, axis), (), 0, length) for axis, length in enumerate(result.shape)]
    main_axis = result.shape.index(max(result.shape))
    next_to = spot[:main_axis] + [(spot[main_axis] + 1) % result.shape[main_axis]] + spot[main_axis + 1:]
    return result.at[tuple(spot)].set(low).at[tuple(next_to)].set(top_value)


def block_scale(key, dims, split, least, high):
    def one(axis_at, blocks):
        steps = jax.random.uniform(jax.random.fold_in(jax.random.fold_in(key, 6), axis_at), (blocks,), jnp.float32, least / len(split), high / len(split))
        return jnp.repeat(jnp.exp(steps), dims[axis_at] // blocks).reshape((-1,) + (1,) * (len(dims) - axis_at - 1))

    gain = one(*split[0])
    for cut in split[1:]:
        gain = gain * one(*cut)
    return gain


def scatter_about(rng, shape, width, reach, shards=(), kind=jnp.bfloat16):
    drawn = width * jax.random.normal(rng, shape, jnp.float32)
    if shards:
        drawn = drawn * block_scale(rng, shape, shards, -0.22, 0.18)
    return jnp.clip(drawn, -reach, reach).astype(kind)


def setup_inputs(seed: int = 0) -> dict:
    seeds = jax.random.split(jax.random.key(seed), 9)
    return {
        "layer_east": scatter_about(seeds[0], (K, NY, NX), 1.0, 6.0, ((0, 2), (1, 4), (2, 4)), jnp.float32),
        "layer_north": scatter_about(seeds[1], (K, NY, NX), 1.0, 6.0, ((0, 2), (1, 4), (2, 4)), jnp.float32),
        "layer_press": scatter_about(seeds[2], (K, NY, NX), 1.0, 6.0, ((0, 2), (1, 4), (2, 4)), jnp.float32),
        "surface": scatter_about(seeds[3], (NY, NX), 0.5, 3.0, ((0, 4), (1, 4)), jnp.float32),
        "land_sea": plant((jax.random.randint(seeds[4], (NY, NX), 0, 8) < 7).astype(jnp.int32), jax.random.fold_in(seeds[4], 1), 0, 1),
        "bottom_level": plant(jax.random.randint(seeds[5], (NY, NX), K - K // 4, K + 1), jax.random.fold_in(seeds[5], 1), K - K // 4, K).astype(jnp.int32),
        "coriolis": jnp.clip(jax.random.uniform(seeds[6], (NY, NX), jnp.float32, -1.0, 1.0) * block_scale(seeds[6], (NY, NX), ((0, 4), (1, 4)), -0.4, 0.0), -1.0, 1.0),
        "level_thick": jnp.clip(jnp.exp(math.log(0.3) - 0.1823216 * jax.random.uniform(seeds[7], (K,), jnp.float32) ** block_scale(seeds[7], (K,), ((0, 2),), -0.2, 0.2)), 0.25, 0.3),
    }


COURANT = 0.25
VISCOSITY = 0.1


def shifted(field, step, axis):
    return jnp.roll(field, -step, axis=axis)


def layer_terms(centre, east, west, north, south, coriolis):
    vel_east, vel_north, press, active = centre
    grad_x = 0.5 * (east[3] * (east[2] - press) + west[3] * (press - west[2]))
    grad_y = 0.5 * (north[3] * (north[2] - press) + south[3] * (press - south[2]))

    def friction(slot, value):
        return (east[3] * (east[slot] - value) + west[3] * (west[slot] - value)
                + north[3] * (north[slot] - value) + south[3] * (south[slot] - value))

    tend_east = active * (-grad_x + coriolis * vel_north + VISCOSITY * friction(0, vel_east))
    tend_north = active * (-grad_y - coriolis * vel_east + VISCOSITY * friction(1, vel_north))
    return tend_east, tend_north


def surface_step(height, trans_east, trans_north, ocean_mid, depth, coriolis, force_east, force_north):
    spread = 0.5 * (trans_east[1:-1, 2:] - trans_east[1:-1, :-2]) + 0.5 * (trans_north[2:, 1:-1] - trans_north[:-2, 1:-1])
    height_mid = ocean_mid * (height[1:-1, 1:-1] - COURANT * spread)
    slope_x = 0.5 * (height_mid[1:-1, 2:] - height_mid[1:-1, :-2])
    slope_y = 0.5 * (height_mid[2:, 1:-1] - height_mid[:-2, 1:-1])
    ocean_core = ocean_mid[1:-1, 1:-1]
    old_east = trans_east[2:-2, 2:-2]
    old_north = trans_north[2:-2, 2:-2]
    new_east = ocean_core * (old_east + COURANT * (-depth * slope_x + coriolis * old_north + force_east))
    new_north = ocean_core * (old_north + COURANT * (-depth * slope_y - coriolis * old_east + force_north))
    return height_mid, new_east, new_north


def reference(layer_east, layer_north, layer_press, surface, land_sea, bottom_level, coriolis, level_thick):
    levels = layer_east.shape[0]
    ocean = land_sea.astype(jnp.float32)
    deepest = ocean * bottom_level.astype(jnp.float32)
    indices = jnp.arange(levels).astype(jnp.float32)[:, None, None]
    active = (indices < deepest[None]).astype(jnp.float32)
    centre = (layer_east, layer_north, layer_press, active)
    east = tuple(shifted(item, 1, 2) for item in centre)
    west = tuple(shifted(item, -1, 2) for item in centre)
    north = tuple(shifted(item, 1, 1) for item in centre)
    south = tuple(shifted(item, -1, 1) for item in centre)
    tend_east, tend_north = layer_terms(centre, east, west, north, south, coriolis)
    thick = level_thick[:, None, None]
    masked_east = active * layer_east
    masked_north = active * layer_north
    force_east = jnp.sum(thick * tend_east, axis=0)
    force_north = jnp.sum(thick * tend_north, axis=0)
    sum_east = jnp.sum(thick * masked_east, axis=0)
    sum_north = jnp.sum(thick * masked_north, axis=0)
    depth = jnp.sum(thick * active, axis=0)
    height, trans_east, trans_north = surface, sum_east, sum_north
    ocean_wide = jnp.pad(ocean, 1, mode="wrap")
    for step in range(SUBSTEPS):
        height_mid, trans_east, trans_north = surface_step(
            jnp.pad(height, 2, mode="wrap"), jnp.pad(trans_east, 2, mode="wrap"),
            jnp.pad(trans_north, 2, mode="wrap"), ocean_wide, depth, coriolis, force_east, force_north)
        height = height_mid[1:-1, 1:-1]
    timestep = SUBSTEPS * COURANT
    floor_depth = depth + (1.0 - ocean)
    east_next = active * (masked_east + timestep * tend_east + (trans_east - sum_east - timestep * force_east) / floor_depth)
    north_next = active * (masked_north + timestep * tend_north + (trans_north - sum_north - timestep * force_north) / floor_depth)
    return height, east_next, north_next
```

```python
import functools

import jax
import jax.numpy as jnp
from jax import lax
from jax.experimental import pallas as pl
from jax.experimental.pallas import tpu as pltpu
from jax.sharding import PartitionSpec as P

SUBSTEPS = 4
COURANT = 0.25
VISCOSITY = 0.1
REACH = 2 * SUBSTEPS
TIMESTEP = SUBSTEPS * COURANT
CHUNK = 2 * REACH

F32 = jnp.float32


class Sizes:
    def __init__(self, levels, rows, cols):
        self.levels = levels
        self.rows = rows
        self.cols = cols
        self.top = 2 * REACH
        self.tall = rows + 4 * REACH
        self.wide = rows + 2 * REACH
        self.slots = cols // REACH
        self.half = cols // 2
        self.planes = 3 * levels + 3
        assert 2 * levels * REACH == cols
        assert rows % CHUNK == 0


def turned(value, shift):
    lanes = value.shape[-1]
    shift = shift % lanes
    if shift == 0:
        return value
    return pltpu.roll(value, shift, axis=1)


def lane_ids(rows, cols):
    return lax.broadcasted_iota(jnp.int32, (rows, cols), 1)


def pack_edges(size, load, rows):
    lane = lane_ids(rows, size.cols)
    slot_of = lane // REACH
    results = []
    for first, count in ((0, 2 * size.levels), (2 * size.levels, size.levels + 3)):
        low = jnp.zeros((rows, size.cols), F32)
        high = jnp.zeros((rows, size.cols), F32)
        for slot in range(count):
            value = turned(load(first + slot), slot * REACH)
            low = jnp.where(slot_of == slot, value, low)
            high = jnp.where(slot_of == (slot - 1) % size.slots, value, high)
        results.append((low, turned(high, REACH)))
    return results


def pack_columns(
    size, east, north, press, surface, land, bottom, coriolis,
    ext, low_out, high_out, whole, sems,
):
    levels, top, rows = size.levels, size.top, size.rows
    span = pl.ds(top, rows)
    copies = []
    for slot, field in enumerate((east, north, press)):
        target = ext.at[pl.ds(slot * levels, levels), span, :]
        copies.append(pltpu.make_async_copy(field, target, sems.at[slot]))
    copies.append(pltpu.make_async_copy(surface, ext.at[3 * levels, span, :], sems.at[3]))
    copies.append(pltpu.make_async_copy(coriolis, ext.at[3 * levels + 2, span, :], sems.at[4]))
    copies.append(pltpu.make_async_copy(land, whole.at[0], sems.at[5]))
    copies.append(pltpu.make_async_copy(bottom, whole.at[1], sems.at[6]))
    for copy in copies:
        copy.start()
    for copy in copies[3:]:
        copy.wait()
    ext[3 * levels + 1, top : top + rows, :] = whole[0].astype(F32) * whole[1].astype(F32)
    for copy in copies[:3]:
        copy.wait()

    @pl.loop(0, rows // CHUNK)
    def _(step):
        start = pl.multiple_of(step * CHUNK, CHUNK)
        packed = pack_edges(size, lambda plane: ext[plane, pl.ds(top + start, CHUNK), :], CHUNK)
        for index, (low, high) in enumerate(packed):
            low_out[index, pl.ds(start, CHUNK), :] = low
            high_out[index, pl.ds(start, CHUNK), :] = high


def pack_rows(size, ext, west, east, south_out, north_out):
    planes, top, rows = size.planes, size.top, size.rows
    south_out[:planes] = ext[:, top : top + REACH, :]
    north_out[:planes] = ext[:, top + rows - REACH : top + rows, :]
    for index, strip in enumerate((west, east)):
        at = planes + 2 * index
        south_out[at : at + 2] = strip[:, :REACH, :]
        north_out[at : at + 2] = strip[:, rows - REACH :, :]


def spread_slot(size, value, slot):
    lane = lane_ids(value.shape[0], size.cols)
    value = jnp.where(lane // REACH == slot, value, 0.0)
    shift = REACH
    while shift < size.cols:
        value = value + turned(value, shift)
        shift *= 2
    return value


def layer_kernel(
    size, thick, ext_in, low, high, west, east, south, north,
    ext, base, sums, statics, strips, own,
):
    del ext_in
    levels, top, rows, cols = size.levels, size.top, size.rows, size.cols
    planes, half = size.planes, size.half
    first_level = (lax.axis_index("gz") * levels).astype(F32)
    below, above = top - REACH, top + rows

    ext[:, below:top, :] = south[:planes]
    ext[:, above : above + REACH, :] = north[:planes]
    VAL, PRS, XVAL, XPRS, CNT, XCNT, COR, RAW = range(8)
    for side, strip in enumerate((west, east)):
        at = planes + 2 * side
        for index, plane in ((0, VAL), (1, RAW)):
            strips[side, plane, below:top, :] = south[at + index]
            strips[side, plane, top:above, :] = strip[index]
            strips[side, plane, above : above + REACH, :] = north[at + index]
    for side, packed in enumerate((low, high)):
        for index in range(2):
            own[side, index, top:above, :] = packed[index]
    for start in (below, above):
        packed = pack_edges(size, lambda plane: ext[plane, start : start + REACH, :], REACH)
        for index in range(2):
            for side in range(2):
                own[side, index, start : start + REACH, :] = packed[index][side]

    @pl.loop(0, size.wide // CHUNK)
    def _(step):
        start = pl.multiple_of(below + step * CHUNK, REACH)
        here = pl.ds(start, CHUNK)
        lane = lane_ids(CHUNK, cols)
        inner = lane % REACH
        for side in range(2):
            edge, toward = ((REACH - 1, -1), (0, 1))[side]
            value, raw = strips[side, VAL, here, :], strips[side, RAW, here, :]

            def beside(array, index):
                mine = turned(own[side, index, here, :], edge if side == 0 else -(REACH - 1))
                return jnp.where(inner == edge, mine, turned(array, toward))

            x_value, x_raw = beside(value, 0), beside(raw, 1)

            def both(array):
                array = jnp.where(lane < half, array, 0.0)
                return array + turned(array, half)

            strips[side, PRS, here, :] = both(raw)
            strips[side, XVAL, here, :] = x_value
            strips[side, XPRS, here, :] = both(x_raw)
            strips[side, CNT, here, :] = spread_slot(size, raw, levels + 1)
            strips[side, XCNT, here, :] = spread_slot(size, jnp.minimum(raw, x_raw), levels + 1)
            strips[side, COR, here, :] = spread_slot(size, raw, levels + 2)
        place = pl.ds(step * CHUNK, CHUNK)
        for index in range(3):
            slot = levels + index
            left = turned(strips[0, RAW, here, :], (size.slots - 1 - slot) * REACH)
            right = turned(strips[1, RAW, here, :], -slot * REACH)
            statics[index, place, :] = jnp.where(
                lane >= cols - REACH, left, jnp.where(lane < REACH, right, 0.0)
            )

    @pl.loop(0, size.wide // CHUNK)
    def _(step):
        start = pl.multiple_of(below + step * CHUNK, REACH)
        here, over, under = (pl.ds(start + move, CHUNK) for move in (0, 1, -1))
        place = pl.ds(step * CHUNK, CHUNK)
        lane = lane_ids(CHUNK, cols)
        slot_of, inner = lane // REACH, lane % REACH
        level_of = (slot_of % levels).astype(F32) + first_level
        eastward = lane < half
        weight = jnp.zeros((CHUNK, cols), F32)
        for k in range(levels):
            weight = jnp.where(slot_of % levels == k, thick[k], weight)

        merged, wet_sides, faces = [], [], []
        for side in range(2):
            value, prs = strips[side, VAL, here, :], strips[side, PRS, here, :]
            cnt, cor = strips[side, CNT, here, :], strips[side, COR, here, :]
            x_value, x_prs = strips[side, XVAL, here, :], strips[side, XPRS, here, :]
            x_wet = level_of < strips[side, XCNT, here, :]
            change = VISCOSITY * (x_value - value)
            push = jnp.where(eastward, 0.5 * (x_prs - prs), 0.0)
            if side == 1:
                change, push = -change, -push
            ahead = jnp.where(x_wet, change - push, 0.0)
            behind = jnp.where(x_wet, change + push, 0.0)
            if side == 0:
                faces.append(behind)
                tend = ahead - turned(behind, 1)
            else:
                faces.append(ahead)
                tend = turned(ahead, -1) - behind
            wet = level_of < cnt
            n_wet = level_of < jnp.minimum(cnt, strips[side, CNT, over, :])
            s_wet = level_of < jnp.minimum(cnt, strips[side, CNT, under, :])
            n_val = jnp.where(n_wet, strips[side, VAL, over, :] - value, 0.0)
            s_val = jnp.where(s_wet, strips[side, VAL, under, :] - value, 0.0)
            n_prs = jnp.where(n_wet, strips[side, PRS, over, :] - prs, 0.0)
            s_prs = jnp.where(s_wet, prs - strips[side, PRS, under, :], 0.0)
            turn = cor * turned(value, half)
            turn = jnp.where(wet, jnp.where(eastward, turn, -turn), 0.0)
            tend = tend + VISCOSITY * (n_val + s_val) + turn
            tend = tend - jnp.where(eastward, 0.0, 0.5 * (n_prs + s_prs))
            force = weight * tend
            total = weight * jnp.where(wet, value, 0.0)
            quarter = half // 2
            force = force + turned(force, quarter)
            total = total + turned(total, -quarter)
            both = jnp.where(lane % half >= quarter, force, total)
            shift = quarter // 2
            while shift >= REACH:
                both = both + turned(both, shift)
                shift //= 2
            merged.append(both)
            wet_sides.append(jnp.where(wet, weight, 0.0))
        deep = jnp.where(eastward, wet_sides[0], wet_sides[1])
        shift = half // 2
        while shift >= REACH:
            deep = deep + turned(deep, shift)
            shift //= 2
        quarter_slots = size.slots // 4
        which = slot_of % quarter_slots
        sums[5, place, :] = jnp.where(
            which == quarter_slots - 1,
            merged[0],
            jnp.where(
                which == quarter_slots - 2,
                turned(merged[1], -REACH),
                turned(deep, -2 * REACH),
            ),
        )
        sides = jnp.where(inner == REACH - 1, faces[0], turned(faces[1], REACH - 2))

        cnt = ext[3 * levels + 1, here, :]
        cor = ext[3 * levels + 2, here, :]
        cnt_x = jnp.minimum(cnt, turned(cnt, -1))
        cnt_n = jnp.minimum(cnt, ext[3 * levels + 1, over, :])
        cnt_s = jnp.minimum(cnt, ext[3 * levels + 1, under, :])
        at_low, at_high = lane == 0, lane == cols - 1
        force_e = force_n = sum_e = sum_n = depth = jnp.zeros((CHUNK, cols), F32)
        for k in range(levels):
            level = first_level + k
            wet, wet_x, wet_n, wet_s = (level < c for c in (cnt, cnt_x, cnt_n, cnt_s))
            u, v, p = (ext[slot * levels + k, here, :] for slot in range(3))
            change_u = jnp.where(wet_x, turned(u, -1) - u, 0.0) * VISCOSITY
            change_v = jnp.where(wet_x, turned(v, -1) - v, 0.0) * VISCOSITY
            push = jnp.where(wet_x, turned(p, -1) - p, 0.0) * 0.5
            side_u = turned(sides, -(k * REACH + REACH - 1))
            side_v = turned(sides, -((levels + k) * REACH + REACH - 1))
            ahead_u = jnp.where(at_high, side_u, change_u - push)
            ahead_v = jnp.where(at_high, side_v, change_v)
            behind_u = jnp.where(at_low, side_u, turned(change_u + push, 1))
            behind_v = jnp.where(at_low, side_v, turned(change_v, 1))

            def vertical(slot, value):
                plane = slot * levels + k
                return (
                    jnp.where(wet_n, ext[plane, over, :] - value, 0.0),
                    jnp.where(wet_s, ext[plane, under, :] - value, 0.0),
                )

            n_u, s_u = vertical(0, u)
            n_v, s_v = vertical(1, v)
            n_p, s_p = vertical(2, p)
            wet_u, wet_v = jnp.where(wet, u, 0.0), jnp.where(wet, v, 0.0)
            tend_e = (ahead_u - behind_u) + cor * wet_v + VISCOSITY * (n_u + s_u)
            tend_n = (
                (ahead_v - behind_v) - cor * wet_u + VISCOSITY * (n_v + s_v) - 0.5 * (n_p - s_p)
            )
            base[0, k, place, :] = wet_u + TIMESTEP * tend_e
            base[1, k, place, :] = wet_v + TIMESTEP * tend_n
            force_e = force_e + thick[k] * tend_e
            force_n = force_n + thick[k] * tend_n
            sum_e = sum_e + thick[k] * wet_u
            sum_n = sum_n + thick[k] * wet_v
            depth = depth + jnp.where(wet, thick[k], 0.0)
        for index, total in enumerate((force_e, force_n, sum_e, sum_n, depth)):
            sums[index, place, :] = total


def surface_kernel(
    size, ext, base, statics, mine, other,
    height_out, east_out, north_out,
    state, fixed, drive, result, sems,
):
    levels, rows, cols, wide = size.levels, size.rows, size.cols, size.wide
    top = size.top
    first_level = (lax.axis_index("gz") * levels).astype(F32)
    lane = lane_ids(CHUNK, cols)
    H, TE, TN = range(3)
    OC, DP, CO, FE, FN = range(5)
    chunks = [REACH + at for at in range(0, wide, CHUNK)]

    @pl.loop(0, wide // CHUNK)
    def _(step):
        place = pl.ds(pl.multiple_of(step * CHUNK, CHUNK), CHUNK)
        here = pl.ds(pl.multiple_of(REACH + step * CHUNK, REACH), CHUNK)
        wider = pl.ds(pl.multiple_of(top - REACH + step * CHUNK, REACH), CHUNK)
        total = [mine[index, place, :] + other[index, place, :] for index in range(6)]
        strip = total[5]
        last = size.slots - 1
        quarter = size.slots // 4

        def outer(left, right):
            return jnp.where(
                lane >= cols - REACH,
                turned(strip, (last - left) * REACH),
                jnp.where(lane < REACH, turned(strip, -right * REACH), 0.0),
            )

        fixed[0, FE, here, :] = total[0]
        fixed[0, FN, here, :] = total[1]
        state[0, TE, here, :] = total[2]
        state[0, TN, here, :] = total[3]
        drive[0, place, :] = total[2] + TIMESTEP * total[0]
        drive[1, place, :] = total[3] + TIMESTEP * total[1]
        fixed[0, DP, here, :] = total[4]
        fixed[1, FE, here, :] = outer(2 * quarter - 1, 2 * quarter - 2)
        fixed[1, FN, here, :] = outer(4 * quarter - 1, 4 * quarter - 2)
        state[1, TE, here, :] = outer(quarter - 1, quarter - 2)
        state[1, TN, here, :] = outer(3 * quarter - 1, 3 * quarter - 2)
        fixed[1, DP, here, :] = outer(2 * quarter - 3, 4 * quarter - 3)
        state[0, H, here, :] = ext[3 * levels, wider, :]
        state[1, H, here, :] = statics[0, place, :]
        fixed[0, OC, here, :] = jnp.where(ext[3 * levels + 1, wider, :] > 0, 1.0, 0.0)
        fixed[1, OC, here, :] = jnp.where(statics[1, place, :] > 0, 1.0, 0.0)
        fixed[0, CO, here, :] = ext[3 * levels + 2, wider, :]
        fixed[1, CO, here, :] = statics[2, place, :]

    def difference_x(field, here):
        inside, outside = state[0, field, here, :], state[1, field, here, :]
        in_e, out_e = turned(inside, -1), turned(outside, -1)
        in_w, out_w = turned(inside, 1), turned(outside, 1)
        at_high, at_low = lane == cols - 1, lane == 0
        return (
            0.5 * (jnp.where(at_high, out_e, in_e) - jnp.where(at_low, out_w, in_w)),
            0.5 * (jnp.where(at_high, in_e, out_e) - jnp.where(at_low, in_w, out_w)),
        )

    def difference_y(part, field, start):
        above = state[part, field, start + 1 : start + 1 + CHUNK, :]
        return 0.5 * (above - state[part, field, start - 1 : start - 1 + CHUNK, :])

    for _ in range(SUBSTEPS):
        for start in chunks:
            here = slice(start, start + CHUNK)
            across = difference_x(TE, here)
            for part in range(2):
                spread = across[part] + difference_y(part, TN, start)
                height = state[part, H, here, :] - COURANT * spread
                state[part, H, here, :] = fixed[part, OC, here, :] * height
        for start in chunks:
            here = slice(start, start + CHUNK)
            across = difference_x(H, here)
            for part in range(2):
                slope_y = difference_y(part, H, start)
                te, tn = state[part, TE, here, :], state[part, TN, here, :]
                oc, dp, co, fe, fn = (fixed[part, index, here, :] for index in range(5))
                state[part, TE, here, :] = oc * (
                    te + COURANT * (-dp * across[part] + co * tn + fe)
                )
                state[part, TN, here, :] = oc * (tn + COURANT * (-dp * slope_y - co * te + fn))

    height_copy = pltpu.make_async_copy(
        state.at[0, H, pl.ds(top, rows), :], height_out, sems.at[0]
    )
    height_copy.start()
    inner = slice(top, top + rows)
    floor_depth = fixed[0, DP, inner, :] + (1.0 - fixed[0, OC, inner, :])
    for index, field in enumerate((TE, TN)):
        gain = state[0, field, inner, :] - drive[index, REACH : REACH + rows, :]
        drive[index, REACH : REACH + rows, :] = gain / floor_depth
    copies = [height_copy]
    for k in range(levels):
        wet = first_level + k < ext[3 * levels + 1, top : top + rows, :]
        for index, out in enumerate((east_out, north_out)):
            change = jnp.where(wet, drive[index, REACH : REACH + rows, :], 0.0)
            result[index, k] = base[index, k, REACH : REACH + rows, :] + change
            copy = pltpu.make_async_copy(
                result.at[index, k], out.at[k], sems.at[1 + 2 * k + index]
            )
            copy.start()
            copies.append(copy)
    for copy in copies:
        copy.wait()


VMEM = pl.BlockSpec(memory_space=pltpu.VMEM)
SMEM = pl.BlockSpec(memory_space=pltpu.SMEM)
HBM = pl.BlockSpec(memory_space=pltpu.HBM)
PARAMS = pltpu.CompilerParams(vmem_limit_bytes=24 * 1024 * 1024)


def shaped(*shape):
    return jax.ShapeDtypeStruct(shape, F32)


def ring(axis):
    count = lax.axis_size(axis)
    forward = [(i, (i + 1) % count) for i in range(count)]
    return forward, [(target, source) for source, target in forward]


def on_device(
    layer_east, layer_north, layer_press, surface, land_sea, bottom_level, coriolis, level_thick
):
    size = Sizes(*layer_east.shape)
    levels, rows, cols = layer_east.shape
    tall, wide = size.tall, size.wide
    ext, low, high = pl.pallas_call(
        functools.partial(pack_columns, size),
        in_specs=[HBM] * 7,
        out_specs=[VMEM] * 3,
        out_shape=[
            shaped(size.planes, tall, cols), shaped(2, rows, cols), shaped(2, rows, cols)
        ],
        scratch_shapes=[
            pltpu.VMEM((2, rows, cols), jnp.int32), pltpu.SemaphoreType.DMA((7,))
        ],
        compiler_params=PARAMS,
        name="pack_columns",
    )(
        *(
            pltpu.with_memory_space_constraint(array, pltpu.HBM)
            for array in (
                layer_east, layer_north, layer_press, surface, land_sea, bottom_level, coriolis
            )
        )
    )
    forward, backward = ring("gx")
    west = lax.ppermute(high, "gx", forward)
    east = lax.ppermute(low, "gx", backward)
    south_out, north_out = pl.pallas_call(
        functools.partial(pack_rows, size),
        in_specs=[VMEM] * 3,
        out_specs=[VMEM] * 2,
        out_shape=[shaped(size.planes + 4, REACH, cols)] * 2,
        compiler_params=PARAMS,
        name="pack_rows",
    )(ext, west, east)
    forward, backward = ring("gy")
    south = lax.ppermute(north_out, "gy", forward)
    north = lax.ppermute(south_out, "gy", backward)
    ext, base, sums, statics = pl.pallas_call(
        functools.partial(layer_kernel, size),
        in_specs=[SMEM] + [VMEM] * 7,
        out_specs=[VMEM] * 4,
        out_shape=[
            shaped(size.planes, tall, cols),
            shaped(2, levels, wide, cols),
            shaped(6, wide, cols),
            shaped(3, wide, cols),
        ],
        scratch_shapes=[
            pltpu.VMEM((2, 8, tall, cols), F32), pltpu.VMEM((2, 2, tall, cols), F32)
        ],
        input_output_aliases={1: 0},
        compiler_params=PARAMS,
        name="layer_terms",
    )(level_thick, ext, low, high, west, east, south, north)
    others = lax.ppermute(sums, "gz", ring("gz")[0])
    height, east_next, north_next = pl.pallas_call(
        functools.partial(surface_kernel, size),
        in_specs=[VMEM] * 5,
        out_specs=[HBM] * 3,
        out_shape=[shaped(rows, cols), shaped(levels, rows, cols), shaped(levels, rows, cols)],
        scratch_shapes=[
            pltpu.VMEM((2, 3, tall, cols), F32),
            pltpu.VMEM((2, 5, tall, cols), F32),
            pltpu.VMEM((2, wide, cols), F32),
            pltpu.VMEM((2, levels, rows, cols), F32),
            pltpu.SemaphoreType.DMA((1 + 2 * levels,)),
        ],
        compiler_params=PARAMS,
        name="surface_steps",
    )(ext, base, statics, sums, others)
    return (height, east_next, north_next)


def solution(mesh):
    return jax.shard_map(
        on_device,
        mesh=mesh,
        in_specs=(
            P("gz", "gy", "gx"),
            P("gz", "gy", "gx"),
            P("gz", "gy", "gx"),
            P("gy", "gx"),
            P("gy", "gx"),
            P("gy", "gx"),
            P("gy", "gx"),
            P("gz"),
        ),
        out_specs=(P("gy", "gx"), P("gz", "gy", "gx"), P("gz", "gy", "gx")),
        check_vma=False,
    )
```

```python
import functools

import jax
import jax.numpy as jnp
from jax import lax
from jax.experimental import pallas as pl
from jax.experimental.pallas import tpu as pltpu
from jax.sharding import PartitionSpec as P


SUBSTEPS = 4
COURANT = 0.25
VISCOSITY = 0.1
REACH = 2 * SUBSTEPS
TIMESTEP = SUBSTEPS * COURANT
CHUNK = 2 * REACH
SIDE_PARTS = 1

F32 = jnp.float32


class Sizes:
    def __init__(self, levels, rows, cols):
        self.levels = levels
        self.rows = rows
        self.cols = cols
        self.wide = rows + 2 * REACH
        self.slots = cols // REACH
        self.half = cols // 2
        self.planes = 3 * levels + 3
        assert 2 * levels * REACH == cols
        assert rows % CHUNK == 0


def turned(value, shift):
    shift = shift % value.shape[-1]
    if shift == 0:
        return value
    return pltpu.roll(value, shift, axis=1)


def repeated(count):
    def run(body):
        for step in range(count):
            body(step)

    return run


def lane_ids(rows, cols):
    return lax.broadcasted_iota(jnp.int32, (rows, cols), 1)


def gathered(value, source):
    return jnp.take_along_axis(value, source, axis=1, mode="promise_in_bounds")


def pairing(axis):
    count = lax.axis_size(axis)
    steps = [(i, (i + 1) % count) for i in range(count)]
    if count % 2:
        return steps, [(target, source) for source, target in steps]
    swaps = [[], []]
    for source, target in steps:
        swaps[source % 2] += [(source, target), (target, source)]
    return swaps


def roles(axis):
    if lax.axis_size(axis) % 2:
        return True, False
    even = lax.axis_index(axis) % 2 == 0
    return even, even


def either(flag, first, second):
    if flag is True:
        return first
    if flag is False:
        return second
    return jnp.where(flag, first, second)


def pack_edges(size, load, rows):
    lane = lane_ids(rows, size.cols)
    slot_of = lane // REACH
    results = []
    for first, count in ((0, 2 * size.levels), (2 * size.levels, size.levels + 3)):
        low = jnp.zeros((rows, size.cols), F32)
        high = jnp.zeros((rows, size.cols), F32)
        for slot in range(count):
            value = turned(load(first + slot), slot * REACH)
            low = jnp.where(slot_of == slot, value, low)
            high = jnp.where(slot_of == (slot - 1) % size.slots, value, high)
        results.append((low, turned(high, REACH)))
    return results


def pack_kernel(
    size, east, north, press, surface, land, bottom, coriolis,
    tile, x_first, x_second, y_first, y_second, whole, sems,
):
    levels, rows = size.levels, size.rows
    copies = []
    for slot, field in enumerate((east, north, press)):
        target = tile.at[pl.ds(slot * levels, levels)]
        copies.append(pltpu.make_async_copy(field, target, sems.at[slot]))
    copies.append(pltpu.make_async_copy(surface, tile.at[3 * levels], sems.at[3]))
    copies.append(pltpu.make_async_copy(coriolis, tile.at[3 * levels + 2], sems.at[4]))
    copies.append(pltpu.make_async_copy(land, whole.at[0], sems.at[5]))
    copies.append(pltpu.make_async_copy(bottom, whole.at[1], sems.at[6]))
    for copy in copies:
        copy.start()
    for copy in copies[3:]:
        copy.wait()
    tile[3 * levels + 1] = whole[0].astype(F32) * whole[1].astype(F32)
    for copy in copies[:3]:
        copy.wait()
    x_flag, _ = roles("gx")
    y_flag, _ = roles("gy")

    def pack(first, second):
        @repeated(rows // CHUNK)
        def _(step):
            here = pl.ds(step * CHUNK, CHUNK)
            packed = pack_edges(size, lambda plane: tile[plane, here, :], CHUNK)
            for index, (low, high) in enumerate(packed):
                first[index, here, :] = either(x_flag, high, low)
                second[index, here, :] = either(x_flag, low, high)

    pack(x_first, x_second)
    low, high = tile[:, :REACH, :], tile[:, rows - REACH :, :]
    y_first[...] = either(y_flag, high, low)
    y_second[...] = either(y_flag, low, high)


def corner_kernel(size, y_first, y_second, base, first, second):
    del base
    x_flag, _ = roles("gx")
    _, north_first = roles("gy")

    def rows_of(plane):
        a, b = y_first[plane], y_second[plane]
        south, north = either(north_first, b, a), either(north_first, a, b)
        return jnp.concatenate([south, north])

    for index, (low, high) in enumerate(pack_edges(size, rows_of, 2 * REACH)):
        first[index] = either(x_flag, high, low)
        second[index] = either(x_flag, low, high)


class Strips:
    def __init__(self, size, thick, rows):
        self.size = size
        self.first_level = (lax.axis_index("gz") * size.levels).astype(F32)
        lane = lane_ids(rows, size.cols)
        self.lane = lane
        self.slot_of, self.inner = lane // REACH, lane % REACH
        self.level_of = (self.slot_of % size.levels).astype(F32) + self.first_level
        self.eastward = lane < size.half
        weight = jnp.zeros((rows, size.cols), F32)
        for k in range(size.levels):
            weight = jnp.where(self.slot_of % size.levels == k, thick[k], weight)
        self.weight = weight

    def slot(self, index):
        return index * REACH + self.inner

    def prepare(self, raw):
        size = self.size
        lane = lane_ids(*raw.shape)
        slot = (size.levels + 1) * REACH + lane % REACH
        return gathered(raw, lane % size.half), gathered(raw, slot)

    def chunk(self, value, raw, own_value, own_raw, around):
        size = self.size
        half, levels = size.half, size.levels
        merged, wet_sides, faces = [], [], []
        for side in range(2):
            edge, toward = ((REACH - 1, -1), (0, 1))[side]

            def beside(array, mine):
                mine = turned(mine, edge if side == 0 else -(REACH - 1))
                return jnp.where(self.inner == edge, mine, turned(array, toward))

            x_value = beside(value[side], own_value[side])
            x_raw = beside(raw[side], own_raw[side])
            x_prs = gathered(x_raw, self.lane % half)
            x_cnt = gathered(jnp.minimum(raw[side], x_raw), self.slot(levels + 1))
            cor = gathered(raw[side], self.slot(levels + 2))
            (val, prs, cnt), over, under = around(side)
            x_wet = self.level_of < x_cnt
            change = VISCOSITY * (x_value - val)
            push = jnp.where(self.eastward, 0.5 * (x_prs - prs), 0.0)
            if side == 1:
                change, push = -change, -push
            ahead = jnp.where(x_wet, change - push, 0.0)
            behind = jnp.where(x_wet, change + push, 0.0)
            if side == 0:
                faces.append(-behind)
                tend = ahead - turned(behind, 1)
            else:
                faces.append(ahead)
                tend = turned(ahead, -1) - behind
            wet = self.level_of < cnt
            n_wet = self.level_of < jnp.minimum(cnt, over[2])
            s_wet = self.level_of < jnp.minimum(cnt, under[2])
            n_val = jnp.where(n_wet, over[0] - val, 0.0)
            s_val = jnp.where(s_wet, under[0] - val, 0.0)
            n_prs = jnp.where(n_wet, over[1] - prs, 0.0)
            s_prs = jnp.where(s_wet, prs - under[1], 0.0)
            turn = cor * turned(val, half)
            turn = jnp.where(wet, jnp.where(self.eastward, turn, -turn), 0.0)
            tend = tend + VISCOSITY * (n_val + s_val) + turn
            tend = tend - jnp.where(self.eastward, 0.0, 0.5 * (n_prs + s_prs))
            force = self.weight * tend
            total = self.weight * jnp.where(wet, val, 0.0)
            quarter = half // 2
            force = force + turned(force, quarter)
            total = total + turned(total, -quarter)
            both = jnp.where(self.lane % half >= quarter, force, total)
            merged.append(self.summed(both, quarter // 2))
            wet_sides.append(jnp.where(wet, self.weight, 0.0))
        deep = self.summed(jnp.where(self.eastward, *wet_sides), half // 2)
        quarter_slots = size.slots // 4
        which = self.slot_of % quarter_slots
        plane = jnp.where(
            which == quarter_slots - 1,
            merged[0],
            jnp.where(
                which == quarter_slots - 2,
                turned(merged[1], -REACH),
                turned(deep, -2 * REACH),
            ),
        )
        sides = jnp.where(self.inner == REACH - 1, faces[0], turned(faces[1], REACH - 2))
        return plane, sides

    def summed(self, value, shift):
        while shift >= REACH:
            value = value + turned(value, shift)
            shift //= 2
        return value

    def at_sides(self, sides, slot):
        rolled = turned(sides, -(slot * REACH + REACH - 1))
        ends = (self.lane == 0) | (self.lane == self.size.cols - 1)
        return jnp.where(ends, rolled, 0.0)

    def side_forces(self, sides):
        levels = self.size.levels
        total = self.summed(self.weight * sides, self.size.half // 2)
        return self.at_sides(total, levels - 1), self.at_sides(total, 2 * levels - 1)

    def statics(self, raw):
        size, results = self.size, []
        for index in range(3):
            slot = size.levels + index
            lane = lane_ids(*raw[0].shape)
            left = turned(raw[0], (size.slots - 1 - slot) * REACH)
            right = turned(raw[1], -slot * REACH)
            results.append(
                jnp.where(
                    lane >= size.cols - REACH, left, jnp.where(lane < REACH, right, 0.0)
                )
            )
        return results


def core_chunk(size, thick, first_level, here, over, under, gains, write):
    levels, cols = size.levels, size.cols
    count = 3 * levels + 1
    cnt, cor = here(count), here(count + 1)
    lane = lane_ids(*cnt.shape)
    cnt_e = jnp.where(lane == cols - 1, -1.0, jnp.minimum(cnt, turned(cnt, -1)))
    cnt_w = jnp.where(lane == 0, -1.0, jnp.minimum(cnt, turned(cnt, 1)))
    cnt_n, cnt_s = jnp.minimum(cnt, over(count)), jnp.minimum(cnt, under(count))
    totals = [jnp.zeros(cnt.shape, F32)] * 5
    for k in range(levels):
        level = first_level + k
        wet, wet_e, wet_w, wet_n, wet_s = (
            level < c for c in (cnt, cnt_e, cnt_w, cnt_n, cnt_s)
        )
        u, v, p = here(k), here(levels + k), here(2 * levels + k)
        slow_u, slow_v, push = VISCOSITY * u, VISCOSITY * v, 0.5 * p
        u_less, u_more = slow_u - push, slow_u + push
        gain_e = jnp.where(wet_e, turned(u_less, -1) - u_less, 0.0)
        gain_e = gain_e + jnp.where(wet_w, turned(u_more, 1) - u_more, 0.0)
        gain_n = jnp.where(wet_e, turned(slow_v, -1) - slow_v, 0.0)
        gain_n = gain_n + jnp.where(wet_w, turned(slow_v, 1) - slow_v, 0.0)
        n_u, s_u = over(k) - u, under(k) - u
        n_v, s_v = over(levels + k) - v, under(levels + k) - v
        n_p, s_p = over(2 * levels + k) - p, p - under(2 * levels + k)
        gain_e = gain_e + VISCOSITY * (jnp.where(wet_n, n_u, 0.0) + jnp.where(wet_s, s_u, 0.0))
        gain_n = gain_n + jnp.where(wet_n, VISCOSITY * n_v - 0.5 * n_p, 0.0)
        gain_n = gain_n + jnp.where(wet_s, VISCOSITY * s_v - 0.5 * s_p, 0.0)
        if gains is not None:
            gain_e, gain_n = gain_e + gains(k), gain_n + gains(levels + k)
        wet_u, wet_v = jnp.where(wet, u, 0.0), jnp.where(wet, v, 0.0)
        tend_e, tend_n = gain_e + cor * wet_v, gain_n - cor * wet_u
        write(0, k, wet_u + TIMESTEP * tend_e)
        write(1, k, wet_v + TIMESTEP * tend_n)
        weight = thick[k]
        parts = (weight * tend_e, weight * tend_n, weight * wet_u, weight * wet_v)
        parts += (jnp.where(wet, weight, 0.0),)
        totals = [total + part for total, part in zip(totals, parts)]
    return totals


def middle_kernel(size, thick, tile, base, sums):
    rows = size.rows
    first_level = (lax.axis_index("gz") * size.levels).astype(F32)

    @repeated((rows - CHUNK) // CHUNK)
    def _(step):
        start = REACH + step * CHUNK

        def load(move):
            return lambda plane: tile[plane, pl.ds(start + move, CHUNK), :]

        def write(field, k, value):
            base[field, k, pl.ds(start, CHUNK), :] = value

        totals = core_chunk(size, thick, first_level, load(0), load(1), load(-1), None, write)
        for index, total in enumerate(totals):
            sums[index, pl.ds(REACH + start, CHUNK), :] = total


def side_kernel(
    size, thick, tile, own_first, own_second, got_first, got_second, sums_in,
    sums, statics, sides_out, work,
):
    rows = size.rows
    high_first, _ = roles("gx")
    _, east_first = roles("gx")
    count = (rows - CHUNK) // SIDE_PARTS
    strips = Strips(size, thick, count)

    def got(index, at):
        a, b = got_first[index, at, :], got_second[index, at, :]
        return either(east_first, b, a), either(east_first, a, b)

    def own(index, at):
        a, b = own_first[index, at, :], own_second[index, at, :]
        return either(high_first, b, a), either(high_first, a, b)

    everything = slice(0, rows)
    value, raw = got(0, everything), got(1, everything)
    place = slice(REACH, REACH + rows)
    for side in range(2):
        work[side, 0] = value[side]
        work[side, 1], work[side, 2] = strips.prepare(raw[side])
    for index, plane in enumerate(strips.statics(raw)):
        statics[index, place, :] = plane
        statics[3 + index, place, :] = tile[3 * size.levels + index]

    for start in range(REACH, rows - REACH, count):
        at, place = slice(start, start + count), slice(start + REACH, start + REACH + count)

        def around(side):
            return [
                [work[side, plane, start + move : start + move + count, :] for plane in range(3)]
                for move in (0, 1, -1)
            ]

        plane, sides = strips.chunk(got(0, at), got(1, at), own(0, at), own(1, at), around)
        sums[5, place, :] = plane
        sides_out[at, :] = sides
        for index, gain in enumerate(strips.side_forces(sides)):
            sums[index, place, :] = sums_in[index, place, :] + gain
        for index in range(2, 5):
            sums[index, place, :] = sums_in[index, place, :]


def outer_kernel(
    size, thick, tile, own_first, own_second, got_first, got_second,
    y_first, y_second, c_first, c_second, c_got_first, c_got_second,
    base_in, sums_in, statics_in,
    base, sums, statics, rows_of, strip_of, own_of,
):
    del base_in, sums_in, statics_in
    rows, planes = size.rows, size.planes
    high_first, east_first = roles("gx")
    _, north_first = roles("gy")
    strips = Strips(size, thick, 2 * CHUNK)
    window = 4 * REACH
    near = (slice(0, CHUNK), slice(rows - CHUNK, rows))
    mine = (slice(CHUNK, window), slice(window, window + CHUNK))
    halo = (slice(REACH, CHUNK), slice(window + CHUNK, window + CHUNK + REACH))

    def outer(plane):
        a, b = y_first[plane], y_second[plane]
        return either(north_first, b, a), either(north_first, a, b)

    def corner(first, second, flag, index):
        a, b = first[index], second[index]
        pair = either(flag, b, a), either(flag, a, b)
        return [(value[:REACH], value[REACH:]) for value in pair]

    def pair_of(first, second, flag, index, at):
        a, b = first[index, at, :], second[index, at, :]
        return either(flag, b, a), either(flag, a, b)

    def joined(ref, lead, move=0):
        return jnp.concatenate(
            [
                ref[(*lead, slice(at + move, at + move + CHUNK), slice(None))]
                for at in (REACH, window + REACH)
            ]
        )

    for plane in range(planes):
        halos = outer(plane)
        for part in range(2):
            rows_of[plane, mine[part], :] = tile[plane, near[part], :]
            rows_of[plane, halo[part], :] = halos[part]
    for index in range(2):
        halos = corner(c_got_first, c_got_second, east_first, index)
        own_halos = corner(c_first, c_second, high_first, index)
        for part in range(2):
            got = pair_of(got_first, got_second, east_first, index, near[part])
            own = pair_of(own_first, own_second, high_first, index, near[part])
            for side in range(2):
                strip_of[side, index, mine[part], :] = got[side]
                strip_of[side, index, halo[part], :] = halos[side][part]
                own_of[side, index, mine[part], :] = own[side]
                own_of[side, index, halo[part], :] = own_halos[side][part]
    for side in range(2):
        strip_of[side, 2], strip_of[side, 3] = strips.prepare(strip_of[side, 1])

    def around(side):
        return [
            [joined(strip_of, (side, plane), move) for plane in (0, 2, 3)] for move in (0, 1, -1)
        ]

    value, raw, own_value, own_raw = (
        [joined(ref, (side, index)) for side in range(2)]
        for ref, index in ((strip_of, 0), (strip_of, 1), (own_of, 0), (own_of, 1))
    )
    places = (slice(0, CHUNK), slice(rows, rows + CHUNK))
    tiles = (slice(0, REACH), slice(rows - REACH, rows))
    kept = (slice(REACH, CHUNK), slice(CHUNK, CHUNK + REACH))

    def store(ref, index, value):
        ref[index, places[0], :] = value[:CHUNK]
        ref[index, places[1], :] = value[CHUNK:]

    plane, sides = strips.chunk(value, raw, own_value, own_raw, around)
    store(sums, 5, plane)
    for index, plane in enumerate(strips.statics(raw)):
        store(statics, index, plane)

    def load(move):
        return lambda plane: joined(rows_of, (plane,), move)

    def write(field, k, value):
        for part in range(2):
            base[field, k, tiles[part], :] = value[kept[part]]

    totals = core_chunk(
        size, thick, strips.first_level, load(0), load(1), load(-1),
        lambda slot: strips.at_sides(sides, slot), write,
    )
    for index, total in enumerate(totals):
        store(sums, index, total)
    for index in range(3):
        store(statics, 3 + index, load(0)(3 * size.levels + index))


def finish_kernel(size, thick, sides_in, base_in, base):
    levels, rows = size.levels, size.rows
    strips = Strips(size, thick, CHUNK)

    @repeated((rows - CHUNK) // CHUNK)
    def _(step):
        at = pl.ds(REACH + step * CHUNK, CHUNK)
        sides = sides_in[at, :]
        for field in range(2):
            for k in range(levels):
                gain = strips.at_sides(sides, field * levels + k)
                base[field, k, at, :] = base_in[field, k, at, :] + TIMESTEP * gain


def surface_kernel(
    size, tile, base, statics, mine, other,
    height_out, east_out, north_out,
    state, fixed, drive, result, sems,
):
    levels, rows, cols, wide = size.levels, size.rows, size.cols, size.wide
    top = 2 * REACH
    first_level = (lax.axis_index("gz") * levels).astype(F32)
    lane = lane_ids(CHUNK, cols)
    H, TE, TN = range(3)
    OC, DP, CO, FE, FN = range(5)
    chunks = [REACH + at for at in range(0, wide, CHUNK)]

    @repeated(wide // CHUNK)
    def _(step):
        place = pl.ds(step * CHUNK, CHUNK)
        here = pl.ds(REACH + step * CHUNK, CHUNK)
        total = [mine[index, place, :] + other[index, place, :] for index in range(6)]
        strip = total[5]
        last = size.slots - 1
        quarter = size.slots // 4

        def outer(left, right):
            return jnp.where(
                lane >= cols - REACH,
                turned(strip, (last - left) * REACH),
                jnp.where(lane < REACH, turned(strip, -right * REACH), 0.0),
            )

        fixed[0, FE, here, :] = total[0]
        fixed[0, FN, here, :] = total[1]
        state[0, TE, here, :] = total[2]
        state[0, TN, here, :] = total[3]
        drive[0, place, :] = total[2] + TIMESTEP * total[0]
        drive[1, place, :] = total[3] + TIMESTEP * total[1]
        fixed[0, DP, here, :] = total[4]
        fixed[1, FE, here, :] = outer(2 * quarter - 1, 2 * quarter - 2)
        fixed[1, FN, here, :] = outer(4 * quarter - 1, 4 * quarter - 2)
        state[1, TE, here, :] = outer(quarter - 1, quarter - 2)
        state[1, TN, here, :] = outer(3 * quarter - 1, 3 * quarter - 2)
        fixed[1, DP, here, :] = outer(2 * quarter - 3, 4 * quarter - 3)
        state[0, H, here, :] = statics[3, place, :]
        state[1, H, here, :] = statics[0, place, :]
        fixed[0, OC, here, :] = jnp.where(statics[4, place, :] > 0, 1.0, 0.0)
        fixed[1, OC, here, :] = jnp.where(statics[1, place, :] > 0, 1.0, 0.0)
        fixed[0, CO, here, :] = statics[5, place, :]
        fixed[1, CO, here, :] = statics[2, place, :]

    def difference_x(field, here):
        inside, outside = state[0, field, here, :], state[1, field, here, :]
        in_e, out_e = turned(inside, -1), turned(outside, -1)
        in_w, out_w = turned(inside, 1), turned(outside, 1)
        at_high, at_low = lane == cols - 1, lane == 0
        return (
            0.5 * (jnp.where(at_high, out_e, in_e) - jnp.where(at_low, out_w, in_w)),
            0.5 * (jnp.where(at_high, in_e, out_e) - jnp.where(at_low, in_w, out_w)),
        )

    def difference_y(part, field, start):
        above = state[part, field, start + 1 : start + 1 + CHUNK, :]
        return 0.5 * (above - state[part, field, start - 1 : start - 1 + CHUNK, :])

    for _ in range(SUBSTEPS):
        for start in chunks:
            here = slice(start, start + CHUNK)
            across = difference_x(TE, here)
            for part in range(2):
                spread = across[part] + difference_y(part, TN, start)
                height = state[part, H, here, :] - COURANT * spread
                state[part, H, here, :] = fixed[part, OC, here, :] * height
        for start in chunks:
            here = slice(start, start + CHUNK)
            across = difference_x(H, here)
            for part in range(2):
                slope_y = difference_y(part, H, start)
                te, tn = state[part, TE, here, :], state[part, TN, here, :]
                oc, dp, co, fe, fn = (fixed[part, index, here, :] for index in range(5))
                state[part, TE, here, :] = oc * (
                    te + COURANT * (-dp * across[part] + co * tn + fe)
                )
                state[part, TN, here, :] = oc * (tn + COURANT * (-dp * slope_y - co * te + fn))

    height_copy = pltpu.make_async_copy(
        state.at[0, H, pl.ds(top, rows), :], height_out, sems.at[0]
    )
    height_copy.start()
    inner = slice(top, top + rows)
    floor_depth = fixed[0, DP, inner, :] + (1.0 - fixed[0, OC, inner, :])
    for index, field in enumerate((TE, TN)):
        gain = state[0, field, inner, :] - drive[index, REACH : REACH + rows, :]
        drive[index, REACH : REACH + rows, :] = gain / floor_depth
    copies = [height_copy]
    for k in range(levels):
        wet = first_level + k < tile[3 * levels + 1]
        for index, out in enumerate((east_out, north_out)):
            change = jnp.where(wet, drive[index, REACH : REACH + rows, :], 0.0)
            result[index, k] = base[index, k] + change
            copy = pltpu.make_async_copy(
                result.at[index, k], out.at[k], sems.at[1 + 2 * k + index]
            )
            copy.start()
            copies.append(copy)
    for copy in copies:
        copy.wait()


VMEM = pl.BlockSpec(memory_space=pltpu.VMEM)
SMEM = pl.BlockSpec(memory_space=pltpu.SMEM)
HBM = pl.BlockSpec(memory_space=pltpu.HBM)


def shaped(*shape):
    return jax.ShapeDtypeStruct(shape, F32)


def call(body, size, ins, outs, shapes, scratch=(), aliases=None, flops=0):
    return pl.pallas_call(
        functools.partial(body, size),
        in_specs=ins,
        out_specs=outs,
        out_shape=shapes,
        scratch_shapes=scratch,
        input_output_aliases=aliases or {},
        compiler_params=pltpu.CompilerParams(vmem_limit_bytes=24 * 1024 * 1024),
        cost_estimate=pl.CostEstimate(flops=flops, bytes_accessed=0, transcendentals=0),
    )


def swapped(axis, first, second):
    pairs = pairing(axis)
    first = lax.ppermute(first, axis, pairs[0])
    second = lax.ppermute(second, axis, pairs[1])
    return first, second


def on_device(
    layer_east, layer_north, layer_press, surface, land_sea, bottom_level, coriolis, level_thick
):
    size = Sizes(*layer_east.shape)
    levels, rows, cols = layer_east.shape
    wide, planes = size.wide, size.planes
    tile, x_first, x_second, y_first, y_second = call(
        pack_kernel,
        size,
        [HBM] * 7,
        [VMEM] * 5,
        [shaped(planes, rows, cols)]
        + [shaped(2, rows, cols)] * 2
        + [shaped(planes, REACH, cols)] * 2,
        [pltpu.VMEM((2, rows, cols), jnp.int32), pltpu.SemaphoreType.DMA((7,))],
    )(
        *(
            pltpu.with_memory_space_constraint(array, pltpu.HBM)
            for array in (
                layer_east, layer_north, layer_press, surface, land_sea, bottom_level, coriolis
            )
        )
    )
    own = x_first, x_second
    got_y = swapped("gy", y_first, y_second)
    got = swapped("gx", *own)
    base, sums = call(
        middle_kernel,
        size,
        [SMEM, VMEM],
        [VMEM] * 2,
        [shaped(2, levels, rows, cols), shaped(6, wide, cols)],
        flops=10**7,
    )(level_thick, tile)
    corners = call(
        corner_kernel, size, [VMEM] * 3, [VMEM] * 2, [shaped(2, 2 * REACH, cols)] * 2
    )(*got_y, base)
    got_corners = swapped("gx", *corners)
    sums, statics, sides = call(
        side_kernel,
        size,
        [SMEM] + [VMEM] * 6,
        [VMEM] * 3,
        [shaped(6, wide, cols), shaped(6, wide, cols), shaped(rows, cols)],
        [pltpu.VMEM((2, 3, rows, cols), F32)],
        {6: 0},
        flops=10**7,
    )(level_thick, tile, *own, *got, sums)
    base, sums, statics = call(
        outer_kernel,
        size,
        [SMEM] + [VMEM] * 14,
        [VMEM] * 3,
        [shaped(2, levels, rows, cols), shaped(6, wide, cols), shaped(6, wide, cols)],
        [
            pltpu.VMEM((planes, 8 * REACH, cols), F32),
            pltpu.VMEM((2, 4, 8 * REACH, cols), F32),
            pltpu.VMEM((2, 2, 8 * REACH, cols), F32),
        ],
        {12: 0, 13: 1, 14: 2},
    )(level_thick, tile, *own, *got, *got_y, *corners, *got_corners, base, sums, statics)
    others = lax.ppermute(sums, "gz", pairing("gz")[0])
    base = call(
        finish_kernel,
        size,
        [SMEM] + [VMEM] * 2,
        [VMEM],
        [shaped(2, levels, rows, cols)],
        aliases={2: 0},
        flops=10**7,
    )(level_thick, sides, base)[0]
    height, east_next, north_next = call(
        surface_kernel,
        size,
        [VMEM] * 5,
        [HBM] * 3,
        [shaped(rows, cols), shaped(levels, rows, cols), shaped(levels, rows, cols)],
        [
            pltpu.VMEM((2, 3, wide + 2 * REACH, cols), F32),
            pltpu.VMEM((2, 5, wide + 2 * REACH, cols), F32),
            pltpu.VMEM((2, wide, cols), F32),
            pltpu.VMEM((2, levels, rows, cols), F32),
            pltpu.SemaphoreType.DMA((1 + 2 * levels,)),
        ],
    )(tile, base, statics, sums, others)
    return (height, east_next, north_next)


def solution(mesh):
    return jax.shard_map(
        on_device,
        mesh=mesh,
        in_specs=(
            P("gz", "gy", "gx"),
            P("gz", "gy", "gx"),
            P("gz", "gy", "gx"),
            P("gy", "gx"),
            P("gy", "gx"),
            P("gy", "gx"),
            P("gy", "gx"),
            P("gz"),
        ),
        out_specs=(P("gy", "gx"), P("gz", "gy", "gx"), P("gz", "gy", "gx")),
        check_vma=False,
    )
```

```python
import functools

import jax
import jax.numpy as jnp
from jax import lax
from jax.experimental import pallas as pl
from jax.experimental.pallas import tpu as pltpu
from jax.sharding import PartitionSpec as P


SUBSTEPS = 4
COURANT = 0.25
VISCOSITY = 0.1
REACH = 2 * SUBSTEPS
TIMESTEP = SUBSTEPS * COURANT
CHUNK = 2 * REACH

F32 = jnp.float32

FIELDS = 8
SURFACE, COUNT, CORIOLIS = 5, 6, 7
SUMS = 5


class Sizes:
    def __init__(self, levels, rows, cols):
        self.levels = levels
        self.rows = rows
        self.cols = cols
        self.wide = rows + 2 * REACH
        self.slots = cols // REACH
        self.half = cols // 2
        assert levels == REACH and self.slots == 2 * FIELDS
        assert rows % CHUNK == 0


def turned(value, shift):
    shift = shift % value.shape[-1]
    if shift == 0:
        return value
    return pltpu.roll(value, shift, axis=1)


def repeated(count):
    def run(body):
        for step in range(count):
            body(step)

    return run


def lane_ids(rows, cols):
    return lax.broadcasted_iota(jnp.int32, (rows, cols), 1)


def gathered(value, source):
    return jnp.take_along_axis(value, source, axis=1, mode="promise_in_bounds")


def pairing(axis):
    count = lax.axis_size(axis)
    steps = [(i, (i + 1) % count) for i in range(count)]
    if count % 2:
        return steps, [(target, source) for source, target in steps]
    swaps = [[], []]
    for source, target in steps:
        swaps[1 - source % 2] += [(source, target), (target, source)]
    return swaps


def roles(axis):
    if lax.axis_size(axis) % 2:
        return True, False
    odd = lax.axis_index(axis) % 2 == 1
    return odd, odd


def either(flag, first, second):
    if flag is True:
        return first
    if flag is False:
        return second
    return jnp.where(flag, first, second)


def pack_lines(size, load, like):
    cols, lane = size.cols, lane_ids(*like)
    low = high = jnp.zeros(like, F32)
    for plane in range(3 * size.levels):
        at = plane // size.levels * 2 * REACH + plane % size.levels
        value = turned(load(plane), at)
        low = jnp.where(lane == at, value, low)
        high = jnp.where(lane == (at - 1) % cols, value, high)
    return low, turned(high, REACH + 1)


def pack_columns(load, lines, like):
    slot_of = lane_ids(*like) // REACH
    low, high = lines
    for index in range(FIELDS):
        value = turned(load(index), (2 * index + 1) * REACH)
        low = jnp.where(slot_of == 2 * index + 1, value, low)
        high = jnp.where(slot_of == 2 * index, value, high)
    return low, high


def shifted_rows(value, shift):
    return pltpu.roll(value, shift % value.shape[0], axis=0)


def row_ids(rows, cols):
    return lax.broadcasted_iota(jnp.int32, (rows, cols), 0)


def split(flag, first, second):
    return either(flag, second, first), either(flag, first, second)


def by_level(thick, index):
    weight = jnp.zeros(index.shape, F32)
    for k in range(REACH):
        weight = jnp.where(index == k, thick[k], weight)
    return weight


def core_chunk(size, thick, first_level, row, here, over, under, cor, write):
    levels, cols = size.levels, size.cols
    count = 3 * levels
    cnt = here(count)
    lane = lane_ids(*cnt.shape)
    cnt_e = jnp.where(lane == cols - 1, -1.0, jnp.minimum(cnt, turned(cnt, -1)))
    cnt_w = jnp.where(lane == 0, -1.0, jnp.minimum(cnt, turned(cnt, 1)))
    cnt_n = jnp.where(row == size.rows - 1, -1.0, jnp.minimum(cnt, over(count)))
    cnt_s = jnp.where(row == 0, -1.0, jnp.minimum(cnt, under(count)))
    totals = [jnp.zeros(cnt.shape, F32)] * 5
    for k in range(levels):
        level = first_level + k
        wet, wet_e, wet_w, wet_n, wet_s = (
            level < c for c in (cnt, cnt_e, cnt_w, cnt_n, cnt_s)
        )
        u, v, p = here(k), here(levels + k), here(2 * levels + k)
        slow_u, slow_v, push = VISCOSITY * u, VISCOSITY * v, 0.5 * p
        u_less, u_more = slow_u - push, slow_u + push
        gain_e = jnp.where(wet_e, turned(u_less, -1) - u_less, 0.0)
        gain_e = gain_e + jnp.where(wet_w, turned(u_more, 1) - u_more, 0.0)
        gain_n = jnp.where(wet_e, turned(slow_v, -1) - slow_v, 0.0)
        gain_n = gain_n + jnp.where(wet_w, turned(slow_v, 1) - slow_v, 0.0)
        n_u, s_u = over(k) - u, under(k) - u
        n_v, s_v = over(levels + k) - v, under(levels + k) - v
        n_p, s_p = over(2 * levels + k) - p, p - under(2 * levels + k)
        gain_e = gain_e + VISCOSITY * (jnp.where(wet_n, n_u, 0.0) + jnp.where(wet_s, s_u, 0.0))
        gain_n = gain_n + jnp.where(wet_n, VISCOSITY * n_v - 0.5 * n_p, 0.0)
        gain_n = gain_n + jnp.where(wet_s, VISCOSITY * s_v - 0.5 * s_p, 0.0)
        wet_u, wet_v = jnp.where(wet, u, 0.0), jnp.where(wet, v, 0.0)
        tend_e, tend_n = gain_e + cor * wet_v, gain_n - cor * wet_u
        if write is not None:
            write(0, k, wet_u + TIMESTEP * tend_e)
            write(1, k, wet_v + TIMESTEP * tend_n)
        weight = thick[k]
        parts = (weight * tend_e, weight * tend_n, weight * wet_u, weight * wet_v)
        parts += (jnp.where(wet, weight, 0.0),)
        totals = [total + part for total, part in zip(totals, parts)]
    return totals


def edge_kernel(
    size, thick_hbm, east, north, press, surface, land, bottom, coriolis,
    y_first, y_second, weights, thick, levels_of, flat, whole, sems,
):
    levels, rows, cols = size.levels, size.rows, size.cols
    first_level = (lax.axis_index("gz") * levels).astype(F32)
    copies = [pltpu.make_async_copy(thick_hbm, thick, sems.at[0])]
    ends = ((0, REACH), (rows - CHUNK, 4 * REACH))
    for part, (source, target) in enumerate(ends):
        span = pl.ds(source, CHUNK)
        for index, array in enumerate((land, bottom)):
            at = whole.at[index, pl.ds(part * CHUNK, CHUNK), :]
            copies.append(pltpu.make_async_copy(array.at[span, :], at, sems.at[len(copies)]))
        for index, array in enumerate((surface, coriolis)):
            at = flat.at[index, pl.ds(target, CHUNK), :]
            copies.append(pltpu.make_async_copy(array.at[span, :], at, sems.at[len(copies)]))
        for slot, array in enumerate((east, north, press)):
            at = levels_of.at[pl.ds(slot * levels, levels), pl.ds(target, CHUNK), :]
            copies.append(pltpu.make_async_copy(array.at[:, span, :], at, sems.at[len(copies)]))
    for copy in copies:
        copy.start()
    for copy in copies:
        copy.wait()
    weights[0] = by_level(thick, row_ids(REACH, cols))
    weights[1] = by_level(thick, lane_ids(REACH, cols) % REACH)
    for part, (_, target) in enumerate(ends):
        span = slice(part * CHUNK, part * CHUNK + CHUNK)
        count = whole[0, span, :].astype(F32) * whole[1, span, :].astype(F32)
        levels_of[3 * levels, target : target + CHUNK, :] = count

    starts = (REACH, 4 * REACH + REACH)

    def joined(ref, plane, move=0):
        return jnp.concatenate([ref[plane, at + move : at + move + REACH, :] for at in starts])

    def load(move):
        return lambda plane: joined(levels_of, plane, move)

    like = (CHUNK, cols)
    row = row_ids(*like)
    row = jnp.where(row < REACH, row, row + rows - CHUNK)
    cor = joined(flat, 1)
    fields = core_chunk(
        size, thick, first_level, row, load(0), load(1), load(-1), cor, None
    )
    fields += [joined(flat, 0), load(0)(3 * levels), cor]
    low, high = pack_lines(size, load(0), like)
    fields.append(low + high)
    y_flag, _ = roles("gy")

    def store(index, south, north):
        y_first[index] = either(y_flag, north, south)
        y_second[index] = either(y_flag, south, north)

    for index, value in enumerate(fields):
        store(index, value[:REACH], value[REACH:])
    for slot in range(3):
        planes = slice(slot * levels, (slot + 1) * levels)
        store(
            FIELDS + 1 + slot,
            *(levels_of[planes, at, :] for at in (REACH, 4 * REACH + CHUNK - 1)),
        )


def tile_kernel(
    size, thick, east, north, press, surface, land, bottom, coriolis, after,
    base, sums, statics, x_first, x_second,
):
    del after
    levels, rows, cols = size.levels, size.rows, size.cols
    first_level = (lax.axis_index("gz") * levels).astype(F32)
    span = slice(REACH, REACH + rows)
    statics[0, span, :] = surface[...]
    statics[1, span, :] = land[...].astype(F32) * bottom[...].astype(F32)
    statics[2, span, :] = coriolis[...]
    fields = (east, north, press)
    x_flag, _ = roles("gx")
    like = (CHUNK, cols)
    for start in range(0, rows, CHUNK):

        def load(move):
            at = start + move

            def value(plane):
                if plane == 3 * levels:
                    return statics[1, REACH + at : REACH + at + CHUNK, :]
                ref, level = fields[plane // levels], plane % levels
                if 0 <= at <= rows - CHUNK:
                    return ref[level, at : at + CHUNK, :]
                return shifted_rows(ref[level, start : start + CHUNK, :], -move)

            return value

        here, place = slice(start, start + CHUNK), slice(start + REACH, start + REACH + CHUNK)

        def write(field, k, value):
            base[field, k, here, :] = value

        totals = core_chunk(
            size, thick, first_level, start + row_ids(*like), load(0), load(1), load(-1),
            statics[2, place, :], write,
        )
        for index, total in enumerate(totals):
            sums[index, place, :] = total
        totals += [statics[index, place, :] for index in range(3)]
        low, high = pack_columns(lambda index: totals[index], pack_lines(size, load(0), like), like)
        x_first[place, :] = either(x_flag, high, low)
        x_second[place, :] = either(x_flag, low, high)


def row_kernel(
    size, weights, own_first, own_second, got_first, got_second,
    sums_in, statics_in, x_first_in, x_second_in,
    sums, statics, x_first, x_second, flux,
):
    del sums_in, statics_in, x_first_in, x_second_in
    levels, rows, cols = size.levels, size.rows, size.cols
    first_level = (lax.axis_index("gz") * levels).astype(F32)
    high_first, north_first = roles("gy")
    x_flag, _ = roles("gx")
    top = REACH + rows
    halo = [split(north_first, got_first[i], got_second[i]) for i in range(FIELDS + 4)]
    mine = [split(high_first, own_first[i], own_second[i]) for i in range(FIELDS + 4)]
    row = row_ids(REACH, cols)
    weight, level_of = weights[0], row.astype(F32) + first_level
    end = REACH - 1
    blocks = [
        [pair[part] for pair in pairs[:FIELDS]]
        for pairs, part in ((halo, 0), (mine, 0), (mine, 1), (halo, 1))
    ]
    lines = [
        pairs[FIELDS][part] for pairs, part in ((halo, 0), (mine, 0), (mine, 1), (halo, 1))
    ]
    for side in range(2):
        south = [(halo[i][0], mine[i][1])[side] for i in range(FIELDS + 4)]
        north = [(mine[i][0], halo[i][1])[side] for i in range(FIELDS + 4)]
        counts = jnp.minimum(south[COUNT][end:, :], north[COUNT][:1, :])
        wet = level_of < jnp.broadcast_to(counts, (REACH, cols))
        change_u, change_v, push = (
            jnp.where(wet, north[FIELDS + 1 + slot] - south[FIELDS + 1 + slot], 0.0)
            for slot in range(3)
        )
        change_u, change_v, push = VISCOSITY * change_u, VISCOSITY * change_v, 0.5 * push
        to_north = (-change_u, -change_v - push)
        to_south = (change_u, change_v - push)
        for field in range(2):
            flux[side, field] = (to_north, to_south)[side][field]
            for block, line, value in (
                (2 * side, end, to_south[field]), (2 * side + 1, 0, to_north[field])
            ):
                gain = jnp.sum(weight * value, axis=0, keepdims=True)
                gain = jnp.where(row == line, jnp.broadcast_to(gain, (REACH, cols)), 0.0)
                blocks[block][field] = blocks[block][field] + gain
    slot_of = lane_ids(REACH, cols) // REACH
    for block, start in enumerate((0, REACH, top - REACH, top)):
        place = slice(start, start + REACH)
        for index in range(SUMS):
            sums[index, place, :] = blocks[block][index]
        for index in range(3):
            statics[index, place, :] = blocks[block][SUMS + index]
        low_line = jnp.where((slot_of < 6) & (slot_of % 2 == 0), lines[block], 0.0)
        high_line = jnp.where((slot_of < 6) & (slot_of % 2 == 1), lines[block], 0.0)
        low, high = pack_columns(
            lambda index: blocks[block][index], (low_line, high_line), (REACH, cols)
        )
        x_first[place, :] = either(x_flag, high, low)
        x_second[place, :] = either(x_flag, low, high)


def column_kernel(
    size, weights, own_first, own_second, got_first, got_second, sums_in,
    sums, flux,
):
    levels, wide, cols = size.levels, size.wide, size.cols
    first_level = (lax.axis_index("gz") * levels).astype(F32)
    high_first, east_first = roles("gx")
    west, east = split(east_first, got_first[...], got_second[...])
    low, high = split(high_first, own_first[...], own_second[...])
    left, right = jnp.concatenate([west, high]), jnp.concatenate([low, east])
    lane = lane_ids(2 * wide, cols)
    slot_of, place = lane // REACH, lane % REACH
    change = turned(right, REACH) - left
    push = turned(change, -4 * REACH)
    counts = jnp.minimum(
        gathered(left, jnp.full_like(lane, (2 * COUNT + 1) * REACH - 1)),
        gathered(right, jnp.full_like(lane, (2 * COUNT + 1) * REACH)),
    )
    wet = (place.astype(F32) + first_level < counts) & ((slot_of == 1) | (slot_of == 3))
    change = jnp.where(wet, VISCOSITY * change, 0.0)
    push = jnp.where(wet & (slot_of == 1), 0.5 * push, 0.0)
    to_east, to_west = -change - push, change - push
    flux[0], flux[1] = to_east[:wide], to_west[wide:]
    weight = jnp.concatenate([weights[1]] * (2 * wide // REACH))
    total = weight * to_east + turned(weight * to_west, size.half)
    for shift in (1, 2, 4):
        total = total + turned(total, shift)
    end = REACH - 1
    at_west, at_east = total[:wide], total[wide:]
    lane = lane_ids(wide, cols)
    for index in range(2):
        source = (2 * index + 1) * REACH + end
        gain = jnp.where(lane == 0, turned(at_west, -source), 0.0)
        gain = gain + jnp.where(
            lane == cols - 1, turned(at_east, cols - 1 - size.half - source), 0.0
        )
        sums[index] = sums_in[index] + gain
    slot_of, place = lane // REACH, lane % REACH
    outer_west = (slot_of == 0) | (slot_of == 2)
    outer_east = (slot_of == 1) | (slot_of == 3)
    gain = jnp.where(
        outer_west & (place == end), turned(at_west, -size.half - REACH), 0.0
    ) + jnp.where(outer_east & (place == 0), turned(at_east, -end), 0.0)
    sums[SUMS] = jnp.where(slot_of % 2 == 0, west, east) + gain


def finish_kernel(size, column_flux, row_flux, base_in, base):
    levels, rows, cols = size.levels, size.rows, size.cols
    lane = lane_ids(CHUNK, cols)
    for start in range(0, rows, CHUNK):
        at = slice(start, start + CHUNK)
        wider = slice(start + REACH, start + REACH + CHUNK)
        west, east = column_flux[0, wider, :], column_flux[1, wider, :]
        for field in range(2):
            for k in range(levels):
                source = (2 * field + 1) * REACH + k
                gain = jnp.where(lane == 0, turned(west, -source), 0.0)
                gain = gain + jnp.where(
                    lane == cols - 1, turned(east, cols - 1 - source), 0.0
                )
                base[field, k, at, :] = base_in[field, k, at, :] + TIMESTEP * gain
    for field in range(2):
        for side, at in enumerate((0, rows - 1)):
            for k in range(levels):
                line = slice(at, at + 1)
                gain = row_flux[side, field, k : k + 1, :]
                base[field, k, line, :] = base[field, k, line, :] + TIMESTEP * gain


def surface_kernel(
    size, base, statics, mine, other,
    height_out, east_out, north_out,
    state, fixed, drive, result, sems,
):
    levels, rows, cols, wide = size.levels, size.rows, size.cols, size.wide
    top = 2 * REACH
    first_level = (lax.axis_index("gz") * levels).astype(F32)
    lane = lane_ids(CHUNK, cols)
    H, TE, TN = range(3)
    OC, DP, CO, FE, FN = range(5)
    chunks = [REACH + at for at in range(0, wide, CHUNK)]

    @repeated(wide // CHUNK)
    def _(step):
        place = pl.ds(step * CHUNK, CHUNK)
        here = pl.ds(REACH + step * CHUNK, CHUNK)
        total = [mine[index, place, :] + other[index, place, :] for index in range(SUMS)]
        strip = mine[SUMS, place, :]
        strip = jnp.where(
            lane < 2 * SUMS * REACH, strip + other[SUMS, place, :], strip
        )

        def outer(index):
            moved = turned(strip, (size.slots - 1 - 2 * index) * REACH)
            return jnp.where((lane < REACH) | (lane >= cols - REACH), moved, 0.0)

        fixed[0, FE, here, :] = total[0]
        fixed[0, FN, here, :] = total[1]
        state[0, TE, here, :] = total[2]
        state[0, TN, here, :] = total[3]
        drive[0, place, :] = total[2] + TIMESTEP * total[0]
        drive[1, place, :] = total[3] + TIMESTEP * total[1]
        fixed[0, DP, here, :] = total[4]
        fixed[1, FE, here, :] = outer(0)
        fixed[1, FN, here, :] = outer(1)
        state[1, TE, here, :] = outer(2)
        state[1, TN, here, :] = outer(3)
        fixed[1, DP, here, :] = outer(4)
        state[0, H, here, :] = statics[0, place, :]
        state[1, H, here, :] = outer(SURFACE)
        fixed[0, OC, here, :] = jnp.where(statics[1, place, :] > 0, 1.0, 0.0)
        fixed[1, OC, here, :] = jnp.where(outer(COUNT) > 0, 1.0, 0.0)
        fixed[0, CO, here, :] = statics[2, place, :]
        fixed[1, CO, here, :] = outer(CORIOLIS)

    def difference_x(field, here):
        inside, outside = state[0, field, here, :], state[1, field, here, :]
        in_e, out_e = turned(inside, -1), turned(outside, -1)
        in_w, out_w = turned(inside, 1), turned(outside, 1)
        at_high, at_low = lane == cols - 1, lane == 0
        return (
            0.5 * (jnp.where(at_high, out_e, in_e) - jnp.where(at_low, out_w, in_w)),
            0.5 * (jnp.where(at_high, in_e, out_e) - jnp.where(at_low, in_w, out_w)),
        )

    def difference_y(part, field, start):
        above = state[part, field, start + 1 : start + 1 + CHUNK, :]
        return 0.5 * (above - state[part, field, start - 1 : start - 1 + CHUNK, :])

    for _ in range(SUBSTEPS):
        for start in chunks:
            here = slice(start, start + CHUNK)
            across = difference_x(TE, here)
            for part in range(2):
                spread = across[part] + difference_y(part, TN, start)
                height = state[part, H, here, :] - COURANT * spread
                state[part, H, here, :] = fixed[part, OC, here, :] * height
        for start in chunks:
            here = slice(start, start + CHUNK)
            across = difference_x(H, here)
            for part in range(2):
                slope_y = difference_y(part, H, start)
                te, tn = state[part, TE, here, :], state[part, TN, here, :]
                oc, dp, co, fe, fn = (fixed[part, index, here, :] for index in range(5))
                state[part, TE, here, :] = oc * (
                    te + COURANT * (-dp * across[part] + co * tn + fe)
                )
                state[part, TN, here, :] = oc * (tn + COURANT * (-dp * slope_y - co * te + fn))

    height_copy = pltpu.make_async_copy(
        state.at[0, H, pl.ds(top, rows), :], height_out, sems.at[0]
    )
    height_copy.start()
    inner = slice(top, top + rows)
    floor_depth = fixed[0, DP, inner, :] + (1.0 - fixed[0, OC, inner, :])
    for index, field in enumerate((TE, TN)):
        gain = state[0, field, inner, :] - drive[index, REACH : REACH + rows, :]
        drive[index, REACH : REACH + rows, :] = gain / floor_depth
    copies = [height_copy]
    for k in range(levels):
        wet = first_level + k < statics[1, REACH : REACH + rows, :]
        for index, out in enumerate((east_out, north_out)):
            change = jnp.where(wet, drive[index, REACH : REACH + rows, :], 0.0)
            result[index, k] = base[index, k] + change
            copy = pltpu.make_async_copy(
                result.at[index, k], out.at[k], sems.at[1 + 2 * k + index]
            )
            copy.start()
            copies.append(copy)
    for copy in copies:
        copy.wait()


VMEM = pl.BlockSpec(memory_space=pltpu.VMEM)
SMEM = pl.BlockSpec(memory_space=pltpu.SMEM)
HBM = pl.BlockSpec(memory_space=pltpu.HBM)


def shaped(*shape):
    return jax.ShapeDtypeStruct(shape, F32)


def call(body, size, ins, outs, shapes, scratch=(), aliases=None, flops=0):
    return pl.pallas_call(
        functools.partial(body, size),
        in_specs=ins,
        out_specs=outs,
        out_shape=shapes,
        scratch_shapes=scratch,
        input_output_aliases=aliases or {},
        compiler_params=pltpu.CompilerParams(vmem_limit_bytes=24 * 1024 * 1024),
        cost_estimate=pl.CostEstimate(flops=flops, bytes_accessed=0, transcendentals=0),
    )


def swapped(axis, first, second):
    pairs = pairing(axis)
    first = lax.ppermute(first, axis, pairs[0])
    second = lax.ppermute(second, axis, pairs[1])
    return first, second


def on_device(
    layer_east, layer_north, layer_press, surface, land_sea, bottom_level, coriolis, level_thick
):
    size = Sizes(*layer_east.shape)
    levels, rows, cols = layer_east.shape
    wide = size.wide
    inputs = [
        pltpu.with_memory_space_constraint(array, pltpu.HBM)
        for array in (
            level_thick, layer_east, layer_north, layer_press,
            surface, land_sea, bottom_level, coriolis,
        )
    ]
    side = shaped(FIELDS + 4, REACH, cols)
    *own_y, weights = call(
        edge_kernel,
        size,
        [HBM] * 8,
        [VMEM] * 3,
        [side, side, shaped(2, REACH, cols)],
        [
            pltpu.SMEM((levels,), F32),
            pltpu.VMEM((3 * levels + 1, 7 * REACH, cols), F32),
            pltpu.VMEM((2, 7 * REACH, cols), F32),
            pltpu.VMEM((2, 2 * CHUNK, cols), jnp.int32),
            pltpu.SemaphoreType.DMA((15,)),
        ],
    )(*inputs)
    got_y = swapped("gy", *own_y)
    base, sums, statics, x_first, x_second = call(
        tile_kernel,
        size,
        [SMEM] + [VMEM] * 8,
        [VMEM] * 5,
        [
            shaped(2, levels, rows, cols),
            shaped(SUMS + 1, wide, cols),
            shaped(3, wide, cols),
            shaped(wide, cols),
            shaped(wide, cols),
        ],
        flops=10**7,
    )(
        level_thick, layer_east, layer_north, layer_press,
        surface, land_sea, bottom_level, coriolis, own_y[0],
    )
    sums, statics, x_first, x_second, row_flux = call(
        row_kernel,
        size,
        [VMEM] * 9,
        [VMEM] * 5,
        [
            shaped(SUMS + 1, wide, cols),
            shaped(3, wide, cols),
            shaped(wide, cols),
            shaped(wide, cols),
            shaped(2, 2, levels, cols),
        ],
        aliases={5: 0, 6: 1, 7: 2, 8: 3},
    )(weights, *own_y, *got_y, sums, statics, x_first, x_second)
    got_x = swapped("gx", x_first, x_second)
    sums, column_flux = call(
        column_kernel,
        size,
        [VMEM] * 6,
        [VMEM] * 2,
        [shaped(SUMS + 1, wide, cols), shaped(2, wide, cols)],
        aliases={5: 0},
    )(weights, x_first, x_second, *got_x, sums)
    others = lax.ppermute(sums, "gz", pairing("gz")[0])
    base = call(
        finish_kernel,
        size,
        [VMEM] * 3,
        [VMEM],
        [shaped(2, levels, rows, cols)],
        aliases={2: 0},
        flops=10**7,
    )(column_flux, row_flux, base)[0]
    height, east_next, north_next = call(
        surface_kernel,
        size,
        [VMEM] * 4,
        [HBM] * 3,
        [shaped(rows, cols), shaped(levels, rows, cols), shaped(levels, rows, cols)],
        [
            pltpu.VMEM((2, 3, wide + 2 * REACH, cols), F32),
            pltpu.VMEM((2, 5, wide + 2 * REACH, cols), F32),
            pltpu.VMEM((2, wide, cols), F32),
            pltpu.VMEM((2, levels, rows, cols), F32),
            pltpu.SemaphoreType.DMA((1 + 2 * levels,)),
        ],
    )(base, statics, sums, others)
    return (height, east_next, north_next)


def solution(mesh):
    return jax.shard_map(
        on_device,
        mesh=mesh,
        in_specs=(
            P("gz", "gy", "gx"),
            P("gz", "gy", "gx"),
            P("gz", "gy", "gx"),
            P("gy", "gx"),
            P("gy", "gx"),
            P("gy", "gx"),
            P("gy", "gx"),
            P("gz"),
        ),
        out_specs=(P("gy", "gx"), P("gz", "gy", "gx"), P("gz", "gy", "gx")),
        check_vma=False,
    )
```

```python
import functools

import jax
import jax.numpy as jnp
from jax import lax
from jax.experimental import pallas as pl
from jax.experimental.pallas import tpu as pltpu
from jax.sharding import PartitionSpec as P


SUBSTEPS = 4
COURANT = 0.25
VISCOSITY = 0.1
REACH = 2 * SUBSTEPS
TIMESTEP = SUBSTEPS * COURANT
CHUNK = 2 * REACH
WAVE = 16

F32 = jnp.float32

FIELDS = 8
SURFACE, COUNT, CORIOLIS = 5, 6, 7
SUMS = 5


class Sizes:
    def __init__(self, levels, rows, cols):
        self.levels = levels
        self.rows = rows
        self.cols = cols
        self.wide = rows + 2 * REACH
        self.slots = cols // REACH
        self.half = cols // 2
        assert levels == REACH and self.slots == 2 * FIELDS
        assert rows % CHUNK == 0


def turned(value, shift):
    shift = shift % value.shape[-1]
    if shift == 0:
        return value
    return pltpu.roll(value, shift, axis=1)


def lane_ids(rows, cols):
    return lax.broadcasted_iota(jnp.int32, (rows, cols), 1)


def gathered(value, source):
    return jnp.take_along_axis(value, source, axis=1, mode="promise_in_bounds")


def pairing(axis):
    count = lax.axis_size(axis)
    steps = [(i, (i + 1) % count) for i in range(count)]
    if count % 2:
        return steps, [(target, source) for source, target in steps]
    swaps = [[], []]
    for source, target in steps:
        swaps[1 - source % 2] += [(source, target), (target, source)]
    return swaps


def roles(axis):
    if lax.axis_size(axis) % 2:
        return True, False
    odd = lax.axis_index(axis) % 2 == 1
    return odd, odd


def either(flag, first, second):
    if flag is True:
        return first
    if flag is False:
        return second
    return jnp.where(flag, first, second)


def pack_lines(size, load, like):
    cols, lane = size.cols, lane_ids(*like)
    low = high = jnp.zeros(like, F32)
    for plane in range(3 * size.levels):
        at = plane // size.levels * 2 * REACH + plane % size.levels
        value = turned(load(plane), at)
        low = jnp.where(lane == at, value, low)
        high = jnp.where(lane == (at - 1) % cols, value, high)
    return low, turned(high, REACH + 1)


def pack_columns(fields, lines, like):
    slot_of = lane_ids(*like) // REACH
    low, high = lines
    for index in range(FIELDS):
        value = turned(fields[index], (2 * index + 1) * REACH)
        low = jnp.where(slot_of == 2 * index + 1, value, low)
        high = jnp.where(slot_of == 2 * index, value, high)
    return low, high


def among(slot_of, slots):
    found = slot_of == slots[0]
    for slot in slots[1:]:
        found = found | (slot_of == slot)
    return found


def shifted_rows(value, shift):
    return pltpu.roll(value, shift % value.shape[0], axis=0)


def row_ids(rows, cols):
    return lax.broadcasted_iota(jnp.int32, (rows, cols), 0)


def split(flag, first, second):
    return either(flag, second, first), either(flag, first, second)


def by_level(thick, index):
    weight = jnp.zeros(index.shape, F32)
    for k in range(REACH):
        weight = jnp.where(index == k, thick[k], weight)
    return weight


def core_chunk(size, weights, first_level, row, here, over, under, cor, write):
    levels, cols = size.levels, size.cols
    count = 3 * levels
    cnt = here(count)
    lane = lane_ids(*cnt.shape)
    cnt_e = jnp.where(lane == cols - 1, -1.0, jnp.minimum(cnt, turned(cnt, -1)))
    cnt_w = jnp.where(lane == 0, -1.0, jnp.minimum(cnt, turned(cnt, 1)))
    cnt_n = jnp.where(row == size.rows - 1, -1.0, jnp.minimum(cnt, over(count)))
    cnt_s = jnp.where(row == 0, -1.0, jnp.minimum(cnt, under(count)))
    totals = [jnp.zeros(cnt.shape, F32)] * 5
    for k in range(levels):
        level = first_level + k
        wet, wet_e, wet_w, wet_n, wet_s = (
            level < c for c in (cnt, cnt_e, cnt_w, cnt_n, cnt_s)
        )
        u, v, p = here(k), here(levels + k), here(2 * levels + k)
        slow_u, slow_v, push = VISCOSITY * u, VISCOSITY * v, 0.5 * p
        u_less, u_more = slow_u - push, slow_u + push
        gain_e = jnp.where(wet_e, turned(u_less, -1) - u_less, 0.0)
        gain_e = gain_e + jnp.where(wet_w, turned(u_more, 1) - u_more, 0.0)
        gain_n = jnp.where(wet_e, turned(slow_v, -1) - slow_v, 0.0)
        gain_n = gain_n + jnp.where(wet_w, turned(slow_v, 1) - slow_v, 0.0)
        n_u, s_u = over(k) - u, under(k) - u
        n_v, s_v = over(levels + k) - v, under(levels + k) - v
        n_p, s_p = over(2 * levels + k) - p, p - under(2 * levels + k)
        gain_e = gain_e + VISCOSITY * (jnp.where(wet_n, n_u, 0.0) + jnp.where(wet_s, s_u, 0.0))
        gain_n = gain_n + jnp.where(wet_n, VISCOSITY * n_v - 0.5 * n_p, 0.0)
        gain_n = gain_n + jnp.where(wet_s, VISCOSITY * s_v - 0.5 * s_p, 0.0)
        wet_u, wet_v = jnp.where(wet, u, 0.0), jnp.where(wet, v, 0.0)
        tend_e, tend_n = gain_e + cor * wet_v, gain_n - cor * wet_u
        if write is not None:
            write(0, k, wet_u + TIMESTEP * tend_e)
            write(1, k, wet_v + TIMESTEP * tend_n)
        weight = weights[k]
        parts = (weight * tend_e, weight * tend_n, weight * wet_u, weight * wet_v)
        parts += (jnp.where(wet, weight, 0.0),)
        totals = [total + part for total, part in zip(totals, parts)]
    return totals


def edge_kernel(
    size, thick_hbm, east, north, press, surface, land, bottom, coriolis,
    y_first, y_second, weights, thick, levels_of, flat, whole, sems,
):
    levels, rows, cols = size.levels, size.rows, size.cols
    first_level = (lax.axis_index("gz") * levels).astype(F32)
    copies = [pltpu.make_async_copy(thick_hbm, thick, sems.at[0])]
    ends = ((0, REACH), (rows - CHUNK, 4 * REACH))
    for source, target in ends:
        span = pl.ds(source, CHUNK)
        for slot, array in enumerate((east, north, press)):
            at = levels_of.at[pl.ds(slot * levels, levels), pl.ds(target, CHUNK), :]
            copies.append(pltpu.make_async_copy(array.at[:, span, :], at, sems.at[len(copies)]))
    for part, (source, target) in enumerate(ends):
        span = pl.ds(source, CHUNK)
        for index, array in enumerate((land, bottom)):
            at = whole.at[index, pl.ds(part * CHUNK, CHUNK), :]
            copies.append(pltpu.make_async_copy(array.at[span, :], at, sems.at[len(copies)]))
        for index, array in enumerate((surface, coriolis)):
            at = flat.at[index, pl.ds(target, CHUNK), :]
            copies.append(pltpu.make_async_copy(array.at[span, :], at, sems.at[len(copies)]))
    for copy in copies:
        copy.start()
    for copy in copies:
        copy.wait()
    weights[0] = by_level(thick, row_ids(REACH, cols))
    weights[1] = by_level(thick, lane_ids(REACH, cols) % REACH)
    for k in range(levels):
        weights[2 + k] = jnp.full((REACH, cols), thick[k])
    for part, (_, target) in enumerate(ends):
        span = slice(part * CHUNK, part * CHUNK + CHUNK)
        count = whole[0, span, :].astype(F32) * whole[1, span, :].astype(F32)
        levels_of[3 * levels, target : target + CHUNK, :] = count

    starts = (REACH, 4 * REACH + REACH)

    def joined(ref, plane, move=0):
        return jnp.concatenate([ref[plane, at + move : at + move + REACH, :] for at in starts])

    def load(move):
        return lambda plane: joined(levels_of, plane, move)

    like = (CHUNK, cols)
    row = row_ids(*like)
    row = jnp.where(row < REACH, row, row + rows - CHUNK)
    cor = joined(flat, 1)
    fields = core_chunk(
        size, thick, first_level, row, load(0), load(1), load(-1), cor, None
    )
    fields += [joined(flat, 0), load(0)(3 * levels), cor]
    low, high = pack_lines(size, load(0), like)
    fields.append(low + high)
    y_flag, _ = roles("gy")

    def store(index, south, north):
        y_first[index] = either(y_flag, north, south)
        y_second[index] = either(y_flag, south, north)

    for index, value in enumerate(fields):
        store(index, value[:REACH], value[REACH:])
    for slot in range(3):
        planes = slice(slot * levels, (slot + 1) * levels)
        store(
            FIELDS + 1 + slot,
            *(levels_of[planes, at, :] for at in (REACH, 4 * REACH + CHUNK - 1)),
        )


def tile_kernel(
    size, weights, east, north, press, surface, land, bottom, coriolis,
    base, sums, statics, x_first, x_second,
):
    levels, rows, cols = size.levels, size.rows, size.cols
    first_level = (lax.axis_index("gz") * levels).astype(F32)
    span = slice(REACH, REACH + rows)
    statics[0, span, :] = surface[...]
    statics[1, span, :] = land[...].astype(F32) * bottom[...].astype(F32)
    statics[2, span, :] = coriolis[...]
    fields = (east, north, press)
    x_flag, _ = roles("gx")
    like = (CHUNK, cols)
    weight = [jnp.concatenate([weights[2 + k]] * (CHUNK // REACH)) for k in range(levels)]
    for start in range(0, rows, CHUNK):

        def load(move):
            at = start + move

            def value(plane):
                if plane == 3 * levels:
                    return statics[1, REACH + at : REACH + at + CHUNK, :]
                ref, level = fields[plane // levels], plane % levels
                if 0 <= at <= rows - CHUNK:
                    return ref[level, at : at + CHUNK, :]
                return shifted_rows(ref[level, start : start + CHUNK, :], -move)

            return value

        here, place = slice(start, start + CHUNK), slice(start + REACH, start + REACH + CHUNK)

        def write(field, k, value):
            base[field, k, here, :] = value

        totals = core_chunk(
            size, weight, first_level, start + row_ids(*like), load(0), load(1), load(-1),
            statics[2, place, :], write,
        )
        for index, total in enumerate(totals):
            sums[index, place, :] = total
        totals += [statics[index, place, :] for index in range(3)]
        low, high = pack_columns(totals, pack_lines(size, load(0), like), like)
        x_first[place, :] = either(x_flag, high, low)
        x_second[place, :] = either(x_flag, low, high)


def row_kernel(
    size, weights, own_first, own_second, got_first, got_second,
    sums_in, statics_in, x_first_in, x_second_in,
    sums, statics, x_first, x_second, flux,
):
    del sums_in, statics_in, x_first_in, x_second_in
    levels, rows, cols = size.levels, size.rows, size.cols
    first_level = (lax.axis_index("gz") * levels).astype(F32)
    high_first, north_first = roles("gy")
    x_flag, _ = roles("gx")
    top = REACH + rows
    halo = [split(north_first, got_first[i], got_second[i]) for i in range(FIELDS + 4)]
    mine = [split(high_first, own_first[i], own_second[i]) for i in range(FIELDS + 4)]
    row = row_ids(REACH, cols)
    weight, level_of = weights[0], row.astype(F32) + first_level
    end = REACH - 1
    blocks = [
        [pair[part] for pair in pairs[:FIELDS]]
        for pairs, part in ((halo, 0), (mine, 0), (mine, 1), (halo, 1))
    ]
    lines = [
        pairs[FIELDS][part] for pairs, part in ((halo, 0), (mine, 0), (mine, 1), (halo, 1))
    ]
    for side in range(2):
        south = [(halo[i][0], mine[i][1])[side] for i in range(FIELDS + 4)]
        north = [(mine[i][0], halo[i][1])[side] for i in range(FIELDS + 4)]
        counts = jnp.minimum(south[COUNT][end:, :], north[COUNT][:1, :])
        wet = level_of < jnp.broadcast_to(counts, (REACH, cols))
        change_u, change_v, push = (
            jnp.where(wet, north[FIELDS + 1 + slot] - south[FIELDS + 1 + slot], 0.0)
            for slot in range(3)
        )
        change_u, change_v, push = VISCOSITY * change_u, VISCOSITY * change_v, 0.5 * push
        to_north = (-change_u, -change_v - push)
        to_south = (change_u, change_v - push)
        for field in range(2):
            flux[side, field] = (to_north, to_south)[side][field]
            for block, line, value in (
                (2 * side, end, to_south[field]), (2 * side + 1, 0, to_north[field])
            ):
                gain = jnp.sum(weight * value, axis=0, keepdims=True)
                gain = jnp.where(row == line, jnp.broadcast_to(gain, (REACH, cols)), 0.0)
                blocks[block][field] = blocks[block][field] + gain
    slot_of = lane_ids(REACH, cols) // REACH
    for block, start in enumerate((0, REACH, top - REACH, top)):
        place = slice(start, start + REACH)
        for index in range(SUMS):
            sums[index, place, :] = blocks[block][index]
        for index in range(3):
            statics[index, place, :] = blocks[block][SUMS + index]
        low_line = jnp.where((slot_of < 6) & (slot_of % 2 == 0), lines[block], 0.0)
        high_line = jnp.where((slot_of < 6) & (slot_of % 2 == 1), lines[block], 0.0)
        low, high = pack_columns(blocks[block], (low_line, high_line), (REACH, cols))
        x_first[place, :] = either(x_flag, high, low)
        x_second[place, :] = either(x_flag, low, high)


def column_kernel(
    size, weights, own_first, own_second, got_first, got_second, ends, flux,
):
    wide, cols, half = size.wide, size.cols, size.half
    first_level = (lax.axis_index("gz") * size.levels).astype(F32)
    high_first, east_first = roles("gx")
    west, east = split(east_first, got_first[...], got_second[...])
    low, high = split(high_first, own_first[...], own_second[...])
    lane = lane_ids(wide, cols)
    slot_of, place = lane // REACH, lane % REACH
    end = REACH - 1
    change = jnp.where(
        lane < half, turned(low, REACH) - west, turned(turned(east, REACH) - high, half)
    )
    count = 2 * COUNT * REACH + end
    counts = jnp.where(
        lane == count, jnp.minimum(west, turned(low, -1)), jnp.minimum(turned(high, 1), east)
    )
    counts = gathered(counts, jnp.where(lane < half, count, count + 1))
    push = turned(change, -4 * REACH)
    eastward = among(slot_of % FIELDS, (1,))
    wet = (place.astype(F32) + first_level < counts) & among(slot_of % FIELDS, (1, 3))
    change = jnp.where(wet, VISCOSITY * change, 0.0)
    push = jnp.where(wet & eastward, 0.5 * push, 0.0)
    to_east, to_west = -change - push, change - push
    flux[0], flux[1] = to_east, to_west
    weight = jnp.concatenate([weights[1]] * (wide // REACH))
    total = weight * to_east + turned(weight * to_west, 4 * REACH)
    for shift in (1, 2, 4):
        total = total + turned(total, shift)
    sources = [(2 * index + 1) * REACH + end for index in range(2)]
    ends[1] = jnp.where(
        among(lane, sources), total, turned(total, -half - 4 * REACH - 1)
    )
    outer_west = among(lane, (end, 2 * REACH + end))
    outer_east = among(lane, (REACH, 3 * REACH))
    gain = jnp.where(outer_west, turned(total, -5 * REACH), 0.0)
    gain = gain + jnp.where(outer_east, turned(total, -half - end), 0.0)
    ends[0] = jnp.where(slot_of % 2 == 0, west, east) + gain


def finish_kernel(size, column_flux, row_flux, base_in, base):
    levels, rows, cols = size.levels, size.rows, size.cols
    lane = lane_ids(CHUNK, cols)
    for start in range(0, rows, CHUNK):
        at = slice(start, start + CHUNK)
        wider = slice(start + REACH, start + REACH + CHUNK)
        west, east = column_flux[0, wider, :], column_flux[1, wider, :]
        for field in range(2):
            for k in range(levels):
                source = (2 * field + 1) * REACH + k
                gain = jnp.where(lane == 0, turned(west, -source), 0.0)
                gain = gain + jnp.where(
                    lane == cols - 1, turned(east, size.half - 1 - source), 0.0
                )
                base[field, k, at, :] = base_in[field, k, at, :] + TIMESTEP * gain
    for field in range(2):
        for side, at in enumerate((0, rows - 1)):
            for k in range(levels):
                line = slice(at, at + 1)
                gain = row_flux[side, field, k : k + 1, :]
                base[field, k, line, :] = base[field, k, line, :] + TIMESTEP * gain


H, TE, TN = range(3)
STEP, SLOPE, TURN, PUSH_E, PUSH_N = range(5)


def coefficients(ocean, depth, coriolis, force_east, force_north):
    step = 0.5 * COURANT * ocean
    twice = COURANT * ocean
    return step, step * depth, twice * coriolis, twice * force_east, twice * force_north


def strip_field(size, strips, index):
    lane = lane_ids(*strips.shape)
    moved = turned(strips, (size.slots - 1 - 2 * index) * REACH)
    return jnp.where((lane < REACH) | (lane >= size.cols - REACH), moved, 0.0)


def blend_kernel(size, mine, other, statics, ends, state, fixed, drive):
    here = slice(REACH, REACH + size.wide)
    total = [mine[index] + other[index] for index in range(SUMS)]
    ocean = jnp.where(statics[1] > 0, 1.0, 0.0)
    values = coefficients(ocean, total[4], statics[2], total[0], total[1])
    for index, value in enumerate(values):
        fixed[0, index, here, :] = value
    for index, value in ((TE, total[2]), (TN, total[3]), (H, ocean * statics[0])):
        state[0, index, here, :] = value
    drive[0] = total[2] + TIMESTEP * total[0]
    drive[1] = total[3] + TIMESTEP * total[1]
    drive[2] = total[4] + (1.0 - ocean)
    strips = ends[0]
    ocean = jnp.where(strip_field(size, strips, COUNT) > 0, 1.0, 0.0)
    fixed[1, STEP, here, :] = 0.5 * COURANT * ocean
    fixed[1, TURN, here, :] = COURANT * ocean * strip_field(size, strips, CORIOLIS)
    state[1, H, here, :] = ocean * strip_field(size, strips, SURFACE)


def surface_kernel(
    size, base, statics, mine, other, state_in, fixed_in, drive_in,
    height_out, east_out, north_out, state, fixed, drive,
    result, sems,
):
    del state_in, fixed_in, drive_in
    levels, rows, cols, wide = size.levels, size.rows, size.cols, size.wide
    top = 2 * REACH
    first_level = (lax.axis_index("gz") * levels).astype(F32)

    here, lane = slice(REACH, REACH + wide), lane_ids(wide, cols)
    strips = mine[0] + other[0]
    force_east, force_north, sum_east, sum_north, depth = (
        strip_field(size, strips, index) for index in range(SUMS)
    )
    step = fixed[1, STEP, here, :]
    fixed[1, SLOPE, here, :] = step * depth
    fixed[1, PUSH_E, here, :] = 2.0 * step * force_east
    fixed[1, PUSH_N, here, :] = 2.0 * step * force_north
    state[1, TE, here, :] = sum_east
    state[1, TN, here, :] = sum_north
    gains = mine[1] + other[1]
    for index, push in ((0, PUSH_E), (1, PUSH_N)):
        gain = turned(gains, -((2 * index + 1) * REACH + REACH - 1))
        gain = jnp.where((lane == 0) | (lane == cols - 1), gain, 0.0)
        fixed[0, push, here, :] = (
            fixed[0, push, here, :] + 2.0 * fixed[0, STEP, here, :] * gain
        )
        drive[index] = drive[index] + TIMESTEP * gain
    lane = lane_ids(WAVE, cols)
    at_high, at_low = lane == cols - 1, lane == 0

    def difference_x(field, here):
        inside, outside = state[0, field, here, :], state[1, field, here, :]
        in_e, out_e = turned(inside, -1), turned(outside, -1)
        in_w, out_w = turned(inside, 1), turned(outside, 1)
        return (
            jnp.where(at_high, out_e, in_e) - jnp.where(at_low, out_w, in_w),
            jnp.where(at_high, in_e, out_e) - jnp.where(at_low, in_w, out_w),
        )

    def difference_y(part, field, start):
        above = state[part, field, start + 1 : start + 1 + WAVE, :]
        return above - state[part, field, start - 1 : start - 1 + WAVE, :]

    def height_part(start):
        here = slice(start, start + WAVE)
        across = difference_x(TE, here)
        for part in range(2):
            spread = across[part] + difference_y(part, TN, start)
            state[part, H, here, :] = (
                state[part, H, here, :] - fixed[part, STEP, here, :] * spread
            )

    def transport_part(start):
        here = slice(start, start + WAVE)
        across = difference_x(H, here)
        for part in range(2):
            slope_y = difference_y(part, H, start)
            te, tn = state[part, TE, here, :], state[part, TN, here, :]
            slope, turn, push_e, push_n = (
                fixed[part, index, here, :] for index in (SLOPE, TURN, PUSH_E, PUSH_N)
            )
            state[part, TE, here, :] = te + (turn * tn + push_e - slope * across[part])
            state[part, TN, here, :] = tn + (push_n - turn * te - slope * slope_y)

    for _ in range(SUBSTEPS):
        for part in (height_part, transport_part):
            for start in range(REACH, REACH + wide, WAVE):
                part(start)

    height_copy = pltpu.make_async_copy(
        state.at[0, H, pl.ds(top, rows), :], height_out, sems.at[0]
    )
    height_copy.start()
    inner = slice(top, top + rows)
    floor_depth = drive[2, REACH : REACH + rows, :]
    for index, field in enumerate((TE, TN)):
        gain = state[0, field, inner, :] - drive[index, REACH : REACH + rows, :]
        drive[index, REACH : REACH + rows, :] = gain / floor_depth
    copies = [height_copy]
    for k in range(levels):
        wet = first_level + k < statics[1, REACH : REACH + rows, :]
        for index, out in enumerate((east_out, north_out)):
            change = jnp.where(wet, drive[index, REACH : REACH + rows, :], 0.0)
            result[index, k] = base[index, k] + change
            copy = pltpu.make_async_copy(
                result.at[index, k], out.at[k], sems.at[1 + 2 * k + index]
            )
            copy.start()
            copies.append(copy)
    for copy in copies:
        copy.wait()


VMEM = pl.BlockSpec(memory_space=pltpu.VMEM)
SMEM = pl.BlockSpec(memory_space=pltpu.SMEM)
HBM = pl.BlockSpec(memory_space=pltpu.HBM)


def shaped(*shape):
    return jax.ShapeDtypeStruct(shape, F32)


def call(body, size, ins, outs, shapes, scratch=(), aliases=None, flops=0):
    return pl.pallas_call(
        functools.partial(body, size),
        in_specs=ins,
        out_specs=outs,
        out_shape=shapes,
        scratch_shapes=scratch,
        input_output_aliases=aliases or {},
        compiler_params=pltpu.CompilerParams(vmem_limit_bytes=24 * 1024 * 1024),
        cost_estimate=pl.CostEstimate(flops=flops, bytes_accessed=0, transcendentals=0),
    )


def swapped(axis, first, second):
    pairs = pairing(axis)
    first = lax.ppermute(first, axis, pairs[0])
    second = lax.ppermute(second, axis, pairs[1])
    return first, second


def on_device(
    layer_east, layer_north, layer_press, surface, land_sea, bottom_level, coriolis, level_thick
):
    size = Sizes(*layer_east.shape)
    levels, rows, cols = layer_east.shape
    wide = size.wide
    inputs = [
        pltpu.with_memory_space_constraint(array, pltpu.HBM)
        for array in (
            level_thick, layer_east, layer_north, layer_press,
            surface, land_sea, bottom_level, coriolis,
        )
    ]
    side = shaped(FIELDS + 4, REACH, cols)
    *own_y, weights = call(
        edge_kernel,
        size,
        [HBM] * 8,
        [VMEM] * 3,
        [side, side, shaped(2 + levels, REACH, cols)],
        [
            pltpu.SMEM((levels,), F32),
            pltpu.VMEM((3 * levels + 1, 7 * REACH, cols), F32),
            pltpu.VMEM((2, 7 * REACH, cols), F32),
            pltpu.VMEM((2, 2 * CHUNK, cols), jnp.int32),
            pltpu.SemaphoreType.DMA((15,)),
        ],
    )(*inputs)
    got_y = swapped("gy", *own_y)
    packed = shaped(wide, cols)
    base, sums, statics, x_first, x_second = call(
        tile_kernel,
        size,
        [VMEM] * 8,
        [VMEM] * 5,
        [
            shaped(2, levels, rows, cols),
            shaped(SUMS, wide, cols),
            shaped(3, wide, cols),
            packed,
            packed,
        ],
        flops=10**7,
    )(
        weights, layer_east, layer_north, layer_press,
        surface, land_sea, bottom_level, coriolis,
    )
    sums, statics, x_first, x_second, row_flux = call(
        row_kernel,
        size,
        [VMEM] * 9,
        [VMEM] * 5,
        [
            shaped(SUMS, wide, cols),
            shaped(3, wide, cols),
            packed,
            packed,
            shaped(2, 2, levels, cols),
        ],
        aliases={5: 0, 6: 1, 7: 2, 8: 3},
    )(weights, *own_y, *got_y, sums, statics, x_first, x_second)
    got_x = swapped("gx", x_first, x_second)
    other_sums = lax.ppermute(sums, "gz", pairing("gz")[0])
    scratch = [
        shaped(2, 3, wide + 2 * REACH, cols),
        shaped(2, 5, wide + 2 * REACH, cols),
        shaped(3, wide, cols),
    ]
    ends, column_flux = call(
        column_kernel,
        size,
        [VMEM] * 5,
        [VMEM] * 2,
        [shaped(2, wide, cols), shaped(2, wide, cols)],
    )(weights, x_first, x_second, *got_x)
    other_ends = lax.ppermute(ends, "gz", pairing("gz")[0])
    blended = call(blend_kernel, size, [VMEM] * 4, [VMEM] * 3, scratch, flops=10**6)(
        sums, other_sums, statics, ends
    )
    base = call(
        finish_kernel,
        size,
        [VMEM] * 3,
        [VMEM],
        [shaped(2, levels, rows, cols)],
        aliases={2: 0},
        flops=10**7,
    )(column_flux, row_flux, base)[0]
    layers = shaped(levels, rows, cols)
    height, east_next, north_next, *_ = call(
        surface_kernel,
        size,
        [VMEM] * 7,
        [HBM] * 3 + [VMEM] * 3,
        [shaped(rows, cols), layers, layers, *scratch],
        [
            pltpu.VMEM((2, levels, rows, cols), F32),
            pltpu.SemaphoreType.DMA((1 + 2 * levels,)),
        ],
        aliases={4: 3, 5: 4, 6: 5},
    )(base, statics, ends, other_ends, *blended)
    return (height, east_next, north_next)


def solution(mesh):
    return jax.shard_map(
        on_device,
        mesh=mesh,
        in_specs=(
            P("gz", "gy", "gx"),
            P("gz", "gy", "gx"),
            P("gz", "gy", "gx"),
            P("gy", "gx"),
            P("gy", "gx"),
            P("gy", "gx"),
            P("gy", "gx"),
            P("gz"),
        ),
        out_specs=(P("gy", "gx"), P("gz", "gy", "gx"), P("gz", "gy", "gx")),
        check_vma=False,
    )
```

```python
import functools

import jax
import jax.numpy as jnp
from jax import lax
from jax.experimental import pallas as pl
from jax.experimental.pallas import tpu as pltpu
from jax.sharding import PartitionSpec as P


SUBSTEPS = 4
COURANT = 0.25
VISCOSITY = 0.1
REACH = 2 * SUBSTEPS
TIMESTEP = SUBSTEPS * COURANT
CHUNK = 2 * REACH
WAVE = 16

F32 = jnp.float32

FIELDS = 8
GAINS = 95
BLOCKS = 2
SURFACE, COUNT, CORIOLIS = 5, 6, 7
SUMS = 5


class Sizes:
    def __init__(self, levels, rows, cols):
        self.levels = levels
        self.rows = rows
        self.cols = cols
        self.wide = rows + 2 * REACH
        self.slots = cols // REACH
        self.half = cols // 2
        assert levels == REACH and self.slots == 2 * FIELDS
        assert rows % CHUNK == 0


def turned(value, shift):
    shift = shift % value.shape[-1]
    if shift == 0:
        return value
    return pltpu.roll(value, shift, axis=1)


def lane_ids(rows, cols):
    return lax.broadcasted_iota(jnp.int32, (rows, cols), 1)


def gathered(value, source):
    return jnp.take_along_axis(value, source, axis=1, mode="promise_in_bounds")


def pairing(axis):
    count = lax.axis_size(axis)
    steps = [(i, (i + 1) % count) for i in range(count)]
    if count % 2:
        return steps, [(target, source) for source, target in steps]
    swaps = [[], []]
    for source, target in steps:
        swaps[1 - source % 2] += [(source, target), (target, source)]
    return swaps


def roles(axis):
    if lax.axis_size(axis) % 2:
        return True, False
    odd = lax.axis_index(axis) % 2 == 1
    return odd, odd


def either(flag, first, second):
    if flag is True:
        return first
    if flag is False:
        return second
    return jnp.where(flag, first, second)


def pack_lines(size, load, like):
    cols, lane = size.cols, lane_ids(*like)
    low = high = jnp.zeros(like, F32)
    for plane in range(3 * size.levels):
        at = plane // size.levels * 2 * REACH + plane % size.levels
        value = turned(load(plane), at)
        low = jnp.where(lane == at, value, low)
        high = jnp.where(lane == (at - 1) % cols, value, high)
    return low, turned(high, REACH + 1)


def pack_columns(fields, lines, like):
    slot_of = lane_ids(*like) // REACH
    low, high = lines
    for index in range(FIELDS):
        value = turned(fields[index], (2 * index + 1) * REACH)
        low = jnp.where(slot_of == 2 * index + 1, value, low)
        high = jnp.where(slot_of == 2 * index, value, high)
    return low, high


def among(slot_of, slots):
    found = slot_of == slots[0]
    for slot in slots[1:]:
        found = found | (slot_of == slot)
    return found


def shifted_rows(value, shift):
    return pltpu.roll(value, shift % value.shape[0], axis=0)


def row_ids(rows, cols):
    return lax.broadcasted_iota(jnp.int32, (rows, cols), 0)


def split(flag, first, second):
    return either(flag, second, first), either(flag, first, second)


def by_level(thick, index):
    weight = jnp.zeros(index.shape, F32)
    for k in range(REACH):
        weight = jnp.where(index == k, thick[k], weight)
    return weight


def core_chunk(size, weights, first_level, row, here, over, under, cor, write):
    levels, cols = size.levels, size.cols
    count = 3 * levels
    cnt = here(count)
    lane = lane_ids(*cnt.shape)
    cnt_e = jnp.where(lane == cols - 1, -1.0, jnp.minimum(cnt, turned(cnt, -1)))
    cnt_w = jnp.where(lane == 0, -1.0, jnp.minimum(cnt, turned(cnt, 1)))
    cnt_n = jnp.where(row == size.rows - 1, -1.0, jnp.minimum(cnt, over(count)))
    cnt_s = jnp.where(row == 0, -1.0, jnp.minimum(cnt, under(count)))
    totals = [jnp.zeros(cnt.shape, F32)] * 5
    for k in range(levels):
        level = first_level + k
        wet, wet_e, wet_w, wet_n, wet_s = (
            level < c for c in (cnt, cnt_e, cnt_w, cnt_n, cnt_s)
        )
        u, v, p = here(k), here(levels + k), here(2 * levels + k)
        slow_u, slow_v, push = VISCOSITY * u, VISCOSITY * v, 0.5 * p
        u_less, u_more = slow_u - push, slow_u + push
        gain_e = jnp.where(wet_e, turned(u_less, -1) - u_less, 0.0)
        gain_e = gain_e + jnp.where(wet_w, turned(u_more, 1) - u_more, 0.0)
        gain_n = jnp.where(wet_e, turned(slow_v, -1) - slow_v, 0.0)
        gain_n = gain_n + jnp.where(wet_w, turned(slow_v, 1) - slow_v, 0.0)
        n_u, s_u = over(k) - u, under(k) - u
        n_v, s_v = over(levels + k) - v, under(levels + k) - v
        n_p, s_p = over(2 * levels + k) - p, p - under(2 * levels + k)
        gain_e = gain_e + VISCOSITY * (jnp.where(wet_n, n_u, 0.0) + jnp.where(wet_s, s_u, 0.0))
        gain_n = gain_n + jnp.where(wet_n, VISCOSITY * n_v - 0.5 * n_p, 0.0)
        gain_n = gain_n + jnp.where(wet_s, VISCOSITY * s_v - 0.5 * s_p, 0.0)
        wet_u, wet_v = jnp.where(wet, u, 0.0), jnp.where(wet, v, 0.0)
        tend_e, tend_n = gain_e + cor * wet_v, gain_n - cor * wet_u
        if write is not None:
            write(0, k, wet_u + TIMESTEP * tend_e)
            write(1, k, wet_v + TIMESTEP * tend_n)
        weight = weights[k]
        parts = (weight * tend_e, weight * tend_n, weight * wet_u, weight * wet_v)
        parts += (jnp.where(wet, weight, 0.0),)
        totals = [total + part for total, part in zip(totals, parts)]
    return totals


def edge_kernel(
    size, thick_hbm, east, north, press, surface, land, bottom, coriolis,
    y_first, y_second, weights, thick, levels_of, flat, whole, sems,
):
    levels, rows, cols = size.levels, size.rows, size.cols
    first_level = (lax.axis_index("gz") * levels).astype(F32)
    copies = [pltpu.make_async_copy(thick_hbm, thick, sems.at[0])]
    ends = ((0, REACH), (rows - CHUNK, 4 * REACH))
    for source, target in ends:
        span = pl.ds(source, CHUNK)
        for slot, array in enumerate((east, north, press)):
            at = levels_of.at[pl.ds(slot * levels, levels), pl.ds(target, CHUNK), :]
            copies.append(pltpu.make_async_copy(array.at[:, span, :], at, sems.at[len(copies)]))
    for part, (source, target) in enumerate(ends):
        span = pl.ds(source, CHUNK)
        for index, array in enumerate((land, bottom)):
            at = whole.at[index, pl.ds(part * CHUNK, CHUNK), :]
            copies.append(pltpu.make_async_copy(array.at[span, :], at, sems.at[len(copies)]))
        for index, array in enumerate((surface, coriolis)):
            at = flat.at[index, pl.ds(target, CHUNK), :]
            copies.append(pltpu.make_async_copy(array.at[span, :], at, sems.at[len(copies)]))
    for copy in copies:
        copy.start()
    for copy in copies:
        copy.wait()
    weights[0] = by_level(thick, row_ids(REACH, cols))
    weights[1] = by_level(thick, lane_ids(REACH, cols) % REACH)
    for k in range(levels):
        weights[2 + k] = jnp.full((REACH, cols), thick[k])
    for part, (_, target) in enumerate(ends):
        span = slice(part * CHUNK, part * CHUNK + CHUNK)
        count = whole[0, span, :].astype(F32) * whole[1, span, :].astype(F32)
        levels_of[3 * levels, target : target + CHUNK, :] = count

    starts = (REACH, 4 * REACH + REACH)

    def joined(ref, plane, move=0):
        return jnp.concatenate([ref[plane, at + move : at + move + REACH, :] for at in starts])

    def load(move):
        return lambda plane: joined(levels_of, plane, move)

    like = (CHUNK, cols)
    row = row_ids(*like)
    row = jnp.where(row < REACH, row, row + rows - CHUNK)
    cor = joined(flat, 1)
    fields = core_chunk(
        size, thick, first_level, row, load(0), load(1), load(-1), cor, None
    )
    fields += [joined(flat, 0), load(0)(3 * levels), cor]
    low, high = pack_lines(size, load(0), like)
    fields.append(low + high)
    y_flag, _ = roles("gy")

    def store(index, south, north):
        y_first[index] = either(y_flag, north, south)
        y_second[index] = either(y_flag, south, north)

    for index, value in enumerate(fields):
        store(index, value[:REACH], value[REACH:])
    for slot in range(3):
        planes = slice(slot * levels, (slot + 1) * levels)
        store(
            FIELDS + 1 + slot,
            *(levels_of[planes, at, :] for at in (REACH, 4 * REACH + CHUNK - 1)),
        )


def tile_kernel(
    size, weights, east, north, press, surface, land, bottom, coriolis,
    base, sums, statics, x_first, x_second, tile, whole, sems,
):
    levels, rows, cols = size.levels, size.rows, size.cols
    first_level = (lax.axis_index("gz") * levels).astype(F32)
    span = pl.ds(REACH, rows)
    flat = [
        pltpu.make_async_copy(land, whole.at[0], sems.at[0]),
        pltpu.make_async_copy(bottom, whole.at[1], sems.at[1]),
        pltpu.make_async_copy(surface, statics.at[0, span, :], sems.at[2]),
        pltpu.make_async_copy(coriolis, statics.at[2, span, :], sems.at[3]),
    ]
    for copy in flat:
        copy.start()
    deep = rows // BLOCKS
    blocks = []
    for block in range(BLOCKS):
        blocks.append([])
        for slot, field in enumerate((east, north, press)):
            at = pl.ds(block * deep, deep)
            copy = pltpu.make_async_copy(
                field.at[:, at, :], tile.at[slot, :, at, :], sems.at[4 + 3 * block + slot]
            )
            copy.start()
            blocks[-1].append(copy)
    for copy in flat:
        copy.wait()
    statics[1, REACH : REACH + rows, :] = whole[0].astype(F32) * whole[1].astype(F32)
    fields = [tile.at[slot] for slot in range(3)]
    arrived = 0
    x_flag, _ = roles("gx")
    like = (CHUNK, cols)
    weight = [jnp.concatenate([weights[2 + k]] * (CHUNK // REACH)) for k in range(levels)]
    for start in range(0, rows, CHUNK):
        while arrived < BLOCKS and arrived * deep < min(start + CHUNK + 1, rows):
            for copy in blocks[arrived]:
                copy.wait()
            arrived += 1

        def load(move):
            at = start + move

            def value(plane):
                if plane == 3 * levels:
                    return statics[1, REACH + at : REACH + at + CHUNK, :]
                ref, level = fields[plane // levels], plane % levels
                if 0 <= at <= rows - CHUNK:
                    return ref[level, at : at + CHUNK, :]
                return shifted_rows(ref[level, start : start + CHUNK, :], -move)

            return value

        here, place = slice(start, start + CHUNK), slice(start + REACH, start + REACH + CHUNK)

        def write(field, k, value):
            base[field, k, here, :] = value

        totals = core_chunk(
            size, weight, first_level, start + row_ids(*like), load(0), load(1), load(-1),
            statics[2, place, :], write,
        )
        for index, total in enumerate(totals):
            sums[index, place, :] = total
        totals += [statics[index, place, :] for index in range(3)]
        low, high = pack_columns(totals, pack_lines(size, load(0), like), like)
        x_first[place, :] = either(x_flag, high, low)
        x_second[place, :] = either(x_flag, low, high)


def row_kernel(
    size, weights, own_first, own_second, got_first, got_second,
    sums_in, statics_in, x_first_in, x_second_in,
    sums, statics, x_first, x_second, flux,
):
    del sums_in, statics_in, x_first_in, x_second_in
    levels, rows, cols = size.levels, size.rows, size.cols
    first_level = (lax.axis_index("gz") * levels).astype(F32)
    high_first, north_first = roles("gy")
    x_flag, _ = roles("gx")
    top = REACH + rows
    halo = [split(north_first, got_first[i], got_second[i]) for i in range(FIELDS + 4)]
    mine = [split(high_first, own_first[i], own_second[i]) for i in range(FIELDS + 4)]
    row = row_ids(REACH, cols)
    weight, level_of = weights[0], row.astype(F32) + first_level
    end = REACH - 1
    blocks = [
        [pair[part] for pair in pairs[:FIELDS]]
        for pairs, part in ((halo, 0), (mine, 0), (mine, 1), (halo, 1))
    ]
    lines = [
        pairs[FIELDS][part] for pairs, part in ((halo, 0), (mine, 0), (mine, 1), (halo, 1))
    ]
    for side in range(2):
        south = [(halo[i][0], mine[i][1])[side] for i in range(FIELDS + 4)]
        north = [(mine[i][0], halo[i][1])[side] for i in range(FIELDS + 4)]
        counts = jnp.minimum(south[COUNT][end:, :], north[COUNT][:1, :])
        wet = level_of < jnp.broadcast_to(counts, (REACH, cols))
        change_u, change_v, push = (
            jnp.where(wet, north[FIELDS + 1 + slot] - south[FIELDS + 1 + slot], 0.0)
            for slot in range(3)
        )
        change_u, change_v, push = VISCOSITY * change_u, VISCOSITY * change_v, 0.5 * push
        to_north = (-change_u, -change_v - push)
        to_south = (change_u, change_v - push)
        for field in range(2):
            flux[side, field] = (to_north, to_south)[side][field]
            for block, line, value in (
                (2 * side, end, to_south[field]), (2 * side + 1, 0, to_north[field])
            ):
                gain = jnp.sum(weight * value, axis=0, keepdims=True)
                gain = jnp.where(row == line, jnp.broadcast_to(gain, (REACH, cols)), 0.0)
                blocks[block][field] = blocks[block][field] + gain
    slot_of = lane_ids(REACH, cols) // REACH
    for block, start in enumerate((0, REACH, top - REACH, top)):
        place = slice(start, start + REACH)
        for index in range(SUMS):
            sums[index, place, :] = blocks[block][index]
        for index in range(3):
            statics[index, place, :] = blocks[block][SUMS + index]
        low_line = jnp.where((slot_of < 6) & (slot_of % 2 == 0), lines[block], 0.0)
        high_line = jnp.where((slot_of < 6) & (slot_of % 2 == 1), lines[block], 0.0)
        low, high = pack_columns(blocks[block], (low_line, high_line), (REACH, cols))
        x_first[place, :] = either(x_flag, high, low)
        x_second[place, :] = either(x_flag, low, high)


def column_kernel(
    size, weights, own_first, own_second, got_first, got_second, ends, strips, flux,
):
    wide, cols, half = size.wide, size.cols, size.half
    first_level = (lax.axis_index("gz") * size.levels).astype(F32)
    high_first, east_first = roles("gx")
    west, east = split(east_first, got_first[...], got_second[...])
    low, high = split(high_first, own_first[...], own_second[...])
    lane = lane_ids(wide, cols)
    slot_of, place = lane // REACH, lane % REACH
    end = REACH - 1
    change = jnp.where(
        lane < half, turned(low, REACH) - west, turned(turned(east, REACH) - high, half)
    )
    count = 2 * COUNT * REACH + end
    counts = jnp.where(
        lane == count, jnp.minimum(west, turned(low, -1)), jnp.minimum(turned(high, 1), east)
    )
    counts = gathered(counts, jnp.where(lane < half, count, count + 1))
    push = turned(change, -4 * REACH)
    eastward = among(slot_of % FIELDS, (1,))
    wet = (place.astype(F32) + first_level < counts) & among(slot_of % FIELDS, (1, 3))
    change = jnp.where(wet, VISCOSITY * change, 0.0)
    push = jnp.where(wet & eastward, 0.5 * push, 0.0)
    to_east, to_west = -change - push, change - push
    flux[0], flux[1] = to_east, to_west
    weight = jnp.concatenate([weights[1]] * (wide // REACH))
    total = weight * to_east + turned(weight * to_west, 4 * REACH)
    for shift in (1, 2, 4):
        total = total + turned(total, shift)
    outer_west = among(lane, (end, 2 * REACH + end))
    outer_east = among(lane, (REACH, 3 * REACH))
    gain = jnp.where(outer_west, turned(total, -5 * REACH), 0.0)
    gain = gain + jnp.where(outer_east, turned(total, -half - end), 0.0)
    strips[...] = jnp.where(slot_of % 2 == 0, west, east)
    for_west = among(lane, [GAINS + 2 * index * REACH for index in range(2)])
    forces = jnp.where(
        for_west, turned(total, GAINS - REACH - end), turned(total, GAINS - half - 6 * REACH)
    )
    ends[...] = jnp.where(lane < 2 * SUMS * REACH, strips[...] + gain, forces)


def finish_kernel(size, column_flux, row_flux, base_in, base):
    levels, rows, cols = size.levels, size.rows, size.cols
    lane = lane_ids(CHUNK, cols)
    for start in range(0, rows, CHUNK):
        at = slice(start, start + CHUNK)
        wider = slice(start + REACH, start + REACH + CHUNK)
        west, east = column_flux[0, wider, :], column_flux[1, wider, :]
        for field in range(2):
            for k in range(levels):
                source = (2 * field + 1) * REACH + k
                gain = jnp.where(lane == 0, turned(west, -source), 0.0)
                gain = gain + jnp.where(
                    lane == cols - 1, turned(east, size.half - 1 - source), 0.0
                )
                base[field, k, at, :] = base_in[field, k, at, :] + TIMESTEP * gain
    for field in range(2):
        for side, at in enumerate((0, rows - 1)):
            for k in range(levels):
                line = slice(at, at + 1)
                gain = row_flux[side, field, k : k + 1, :]
                base[field, k, line, :] = base[field, k, line, :] + TIMESTEP * gain


H, TE, TN = range(3)
STEP, SLOPE, TURN, PUSH_E, PUSH_N = range(5)


def coefficients(ocean, depth, coriolis, force_east, force_north):
    step = 0.5 * COURANT * ocean
    twice = COURANT * ocean
    return step, step * depth, twice * coriolis, twice * force_east, twice * force_north


def strip_field(size, strips, index):
    lane = lane_ids(*strips.shape)
    moved = turned(strips, (size.slots - 1 - 2 * index) * REACH)
    return jnp.where((lane < REACH) | (lane >= size.cols - REACH), moved, 0.0)


def blend_kernel(size, mine, other, statics, strips, state, fixed, drive):
    here = slice(REACH, REACH + size.wide)
    total = [mine[index] + other[index] for index in range(SUMS)]
    ocean = jnp.where(statics[1] > 0, 1.0, 0.0)
    values = coefficients(ocean, total[4], statics[2], total[0], total[1])
    for index, value in enumerate(values):
        fixed[0, index, here, :] = value
    for index, value in ((TE, total[2]), (TN, total[3]), (H, ocean * statics[0])):
        state[0, index, here, :] = value
    drive[0] = total[2] + TIMESTEP * total[0]
    drive[1] = total[3] + TIMESTEP * total[1]
    drive[2] = total[4] + (1.0 - ocean)
    strips = strips[...]
    ocean = jnp.where(strip_field(size, strips, COUNT) > 0, 1.0, 0.0)
    fixed[1, STEP, here, :] = 0.5 * COURANT * ocean
    fixed[1, TURN, here, :] = COURANT * ocean * strip_field(size, strips, CORIOLIS)
    state[1, H, here, :] = ocean * strip_field(size, strips, SURFACE)


def surface_kernel(
    size, base, statics, mine, other, state_in, fixed_in, drive_in,
    height_out, east_out, north_out, state, fixed, drive,
    result, sems,
):
    del state_in, fixed_in, drive_in
    levels, rows, cols, wide = size.levels, size.rows, size.cols, size.wide
    top = 2 * REACH
    first_level = (lax.axis_index("gz") * levels).astype(F32)

    here, lane = slice(REACH, REACH + wide), lane_ids(wide, cols)
    strips = mine[...] + other[...]
    force_east, force_north, sum_east, sum_north, depth = (
        strip_field(size, strips, index) for index in range(SUMS)
    )
    step = fixed[1, STEP, here, :]
    fixed[1, SLOPE, here, :] = step * depth
    fixed[1, PUSH_E, here, :] = 2.0 * step * force_east
    fixed[1, PUSH_N, here, :] = 2.0 * step * force_north
    state[1, TE, here, :] = sum_east
    state[1, TN, here, :] = sum_north
    for index, push in ((0, PUSH_E), (1, PUSH_N)):
        gain = turned(strips, -GAINS - 2 * index * REACH)
        gain = jnp.where((lane == 0) | (lane == cols - 1), gain, 0.0)
        fixed[0, push, here, :] = (
            fixed[0, push, here, :] + 2.0 * fixed[0, STEP, here, :] * gain
        )
        drive[index] = drive[index] + TIMESTEP * gain
    lane = lane_ids(WAVE, cols)
    at_high, at_low = lane == cols - 1, lane == 0

    def difference_x(field, here):
        inside, outside = state[0, field, here, :], state[1, field, here, :]
        in_e, out_e = turned(inside, -1), turned(outside, -1)
        in_w, out_w = turned(inside, 1), turned(outside, 1)
        return (
            jnp.where(at_high, out_e, in_e) - jnp.where(at_low, out_w, in_w),
            jnp.where(at_high, in_e, out_e) - jnp.where(at_low, in_w, out_w),
        )

    def difference_y(part, field, start):
        above = state[part, field, start + 1 : start + 1 + WAVE, :]
        return above - state[part, field, start - 1 : start - 1 + WAVE, :]

    def height_part(start):
        here = slice(start, start + WAVE)
        across = difference_x(TE, here)
        for part in range(2):
            spread = across[part] + difference_y(part, TN, start)
            state[part, H, here, :] = (
                state[part, H, here, :] - fixed[part, STEP, here, :] * spread
            )

    def transport_part(start):
        here = slice(start, start + WAVE)
        across = difference_x(H, here)
        for part in range(2):
            slope_y = difference_y(part, H, start)
            te, tn = state[part, TE, here, :], state[part, TN, here, :]
            slope, turn, push_e, push_n = (
                fixed[part, index, here, :] for index in (SLOPE, TURN, PUSH_E, PUSH_N)
            )
            state[part, TE, here, :] = te + (turn * tn + push_e - slope * across[part])
            state[part, TN, here, :] = tn + (push_n - turn * te - slope * slope_y)

    for _ in range(SUBSTEPS):
        for part in (height_part, transport_part):
            for start in range(REACH, REACH + wide, WAVE):
                part(start)

    height_copy = pltpu.make_async_copy(
        state.at[0, H, pl.ds(top, rows), :], height_out, sems.at[0]
    )
    height_copy.start()
    inner = slice(top, top + rows)
    floor_depth = drive[2, REACH : REACH + rows, :]
    for index, field in enumerate((TE, TN)):
        gain = state[0, field, inner, :] - drive[index, REACH : REACH + rows, :]
        drive[index, REACH : REACH + rows, :] = gain / floor_depth
    copies = [height_copy]
    for k in range(levels):
        wet = first_level + k < statics[1, REACH : REACH + rows, :]
        for index, out in enumerate((east_out, north_out)):
            change = jnp.where(wet, drive[index, REACH : REACH + rows, :], 0.0)
            result[index, k] = base[index, k] + change
            copy = pltpu.make_async_copy(
                result.at[index, k], out.at[k], sems.at[1 + 2 * k + index]
            )
            copy.start()
            copies.append(copy)
    for copy in copies:
        copy.wait()


VMEM = pl.BlockSpec(memory_space=pltpu.VMEM)
SMEM = pl.BlockSpec(memory_space=pltpu.SMEM)
HBM = pl.BlockSpec(memory_space=pltpu.HBM)


def shaped(*shape):
    return jax.ShapeDtypeStruct(shape, F32)


def call(body, size, ins, outs, shapes, scratch=(), aliases=None, flops=0):
    return pl.pallas_call(
        functools.partial(body, size),
        in_specs=ins,
        out_specs=outs,
        out_shape=shapes,
        scratch_shapes=scratch,
        input_output_aliases=aliases or {},
        compiler_params=pltpu.CompilerParams(vmem_limit_bytes=24 * 1024 * 1024),
        cost_estimate=pl.CostEstimate(flops=flops, bytes_accessed=0, transcendentals=0),
    )


def swapped(axis, first, second):
    pairs = pairing(axis)
    first = lax.ppermute(first, axis, pairs[0])
    second = lax.ppermute(second, axis, pairs[1])
    return first, second


def on_device(
    layer_east, layer_north, layer_press, surface, land_sea, bottom_level, coriolis, level_thick
):
    size = Sizes(*layer_east.shape)
    levels, rows, cols = layer_east.shape
    wide = size.wide
    inputs = [
        pltpu.with_memory_space_constraint(array, pltpu.HBM)
        for array in (
            level_thick, layer_east, layer_north, layer_press,
            surface, land_sea, bottom_level, coriolis,
        )
    ]
    side = shaped(FIELDS + 4, REACH, cols)
    *own_y, weights = call(
        edge_kernel,
        size,
        [HBM] * 8,
        [VMEM] * 3,
        [side, side, shaped(2 + levels, REACH, cols)],
        [
            pltpu.SMEM((levels,), F32),
            pltpu.VMEM((3 * levels + 1, 7 * REACH, cols), F32),
            pltpu.VMEM((2, 7 * REACH, cols), F32),
            pltpu.VMEM((2, 2 * CHUNK, cols), jnp.int32),
            pltpu.SemaphoreType.DMA((15,)),
        ],
    )(*inputs)
    got_y = swapped("gy", *own_y)
    packed = shaped(wide, cols)
    base, sums, statics, x_first, x_second = call(
        tile_kernel,
        size,
        [VMEM] + [HBM] * 7,
        [VMEM] * 5,
        [
            shaped(2, levels, rows, cols),
            shaped(SUMS, wide, cols),
            shaped(3, wide, cols),
            packed,
            packed,
        ],
        [
            pltpu.VMEM((3, levels, rows, cols), F32),
            pltpu.VMEM((2, rows, cols), jnp.int32),
            pltpu.SemaphoreType.DMA((4 + 3 * BLOCKS,)),
        ],
        flops=10**7,
    )(weights, *inputs[1:])
    sums, statics, x_first, x_second, row_flux = call(
        row_kernel,
        size,
        [VMEM] * 9,
        [VMEM] * 5,
        [
            shaped(SUMS, wide, cols),
            shaped(3, wide, cols),
            packed,
            packed,
            shaped(2, 2, levels, cols),
        ],
        aliases={5: 0, 6: 1, 7: 2, 8: 3},
    )(weights, *own_y, *got_y, sums, statics, x_first, x_second)
    got_x = swapped("gx", x_first, x_second)
    other_sums = lax.ppermute(sums, "gz", pairing("gz")[0])
    scratch = [
        shaped(2, 3, wide + 2 * REACH, cols),
        shaped(2, 5, wide + 2 * REACH, cols),
        shaped(3, wide, cols),
    ]
    ends, strips, column_flux = call(
        column_kernel,
        size,
        [VMEM] * 5,
        [VMEM] * 3,
        [packed, packed, shaped(2, wide, cols)],
    )(weights, x_first, x_second, *got_x)
    other_ends = lax.ppermute(ends, "gz", pairing("gz")[0])
    blended = call(blend_kernel, size, [VMEM] * 4, [VMEM] * 3, scratch, flops=10**6)(
        sums, other_sums, statics, strips
    )
    base = call(
        finish_kernel,
        size,
        [VMEM] * 3,
        [VMEM],
        [shaped(2, levels, rows, cols)],
        aliases={2: 0},
        flops=10**7,
    )(column_flux, row_flux, base)[0]
    layers = shaped(levels, rows, cols)
    height, east_next, north_next, *_ = call(
        surface_kernel,
        size,
        [VMEM] * 7,
        [HBM] * 3 + [VMEM] * 3,
        [shaped(rows, cols), layers, layers, *scratch],
        [
            pltpu.VMEM((2, levels, rows, cols), F32),
            pltpu.SemaphoreType.DMA((1 + 2 * levels,)),
        ],
        aliases={4: 3, 5: 4, 6: 5},
    )(base, statics, ends, other_ends, *blended)
    return (height, east_next, north_next)


def solution(mesh):
    return jax.shard_map(
        on_device,
        mesh=mesh,
        in_specs=(
            P("gz", "gy", "gx"),
            P("gz", "gy", "gx"),
            P("gz", "gy", "gx"),
            P("gy", "gx"),
            P("gy", "gx"),
            P("gy", "gx"),
            P("gy", "gx"),
            P("gz"),
        ),
        out_specs=(P("gy", "gx"), P("gz", "gy", "gx"), P("gz", "gy", "gx")),
        check_vma=False,
    )
```

```python
import functools

import jax
import jax.numpy as jnp
from jax import lax
from jax.experimental import pallas as pl
from jax.experimental.pallas import tpu as pltpu
from jax.sharding import PartitionSpec as P


SUBSTEPS = 4
COURANT = 0.25
VISCOSITY = 0.1
REACH = 2 * SUBSTEPS
TIMESTEP = SUBSTEPS * COURANT
CHUNK = 2 * REACH
WAVE = 16

F32 = jnp.float32

FIELDS = 8
GAINS = 95
SURFACE, COUNT, CORIOLIS = 5, 6, 7
SUMS = 5


class Sizes:
    def __init__(self, levels, rows, cols):
        self.levels = levels
        self.rows = rows
        self.cols = cols
        self.wide = rows + 2 * REACH
        self.slots = cols // REACH
        self.half = cols // 2
        assert levels == REACH and self.slots == 2 * FIELDS
        assert rows % CHUNK == 0


def turned(value, shift):
    shift = shift % value.shape[-1]
    if shift == 0:
        return value
    return pltpu.roll(value, shift, axis=1)


def lane_ids(rows, cols):
    return lax.broadcasted_iota(jnp.int32, (rows, cols), 1)


def gathered(value, source):
    return jnp.take_along_axis(value, source, axis=1, mode="promise_in_bounds")


def pairing(axis):
    count = lax.axis_size(axis)
    steps = [(i, (i + 1) % count) for i in range(count)]
    if count % 2:
        return steps, [(target, source) for source, target in steps]
    swaps = [[], []]
    for source, target in steps:
        swaps[1 - source % 2] += [(source, target), (target, source)]
    return swaps


def roles(axis):
    if lax.axis_size(axis) % 2:
        return True, False
    odd = lax.axis_index(axis) % 2 == 1
    return odd, odd


def either(flag, first, second):
    if flag is True:
        return first
    if flag is False:
        return second
    return jnp.where(flag, first, second)


def pack_lines(size, load, like):
    cols, lane = size.cols, lane_ids(*like)
    low = high = jnp.zeros(like, F32)
    for plane in range(3 * size.levels):
        at = plane // size.levels * 2 * REACH + plane % size.levels
        value = turned(load(plane), at)
        low = jnp.where(lane == at, value, low)
        high = jnp.where(lane == (at - 1) % cols, value, high)
    return low, turned(high, REACH + 1)


def pack_columns(fields, lines, like):
    slot_of = lane_ids(*like) // REACH
    low, high = lines
    for index in range(FIELDS):
        value = turned(fields[index], (2 * index + 1) * REACH)
        low = jnp.where(slot_of == 2 * index + 1, value, low)
        high = jnp.where(slot_of == 2 * index, value, high)
    return low, high


def among(slot_of, slots):
    found = slot_of == slots[0]
    for slot in slots[1:]:
        found = found | (slot_of == slot)
    return found


def shifted_rows(value, shift):
    return pltpu.roll(value, shift % value.shape[0], axis=0)


def row_ids(rows, cols):
    return lax.broadcasted_iota(jnp.int32, (rows, cols), 0)


def split(flag, first, second):
    return either(flag, second, first), either(flag, first, second)


def by_level(thick, index):
    weight = jnp.zeros(index.shape, F32)
    for k in range(REACH):
        weight = jnp.where(index == k, thick[k], weight)
    return weight


def core_chunk(size, weights, first_level, row, here, over, under, cor, write):
    levels, cols = size.levels, size.cols
    count = 3 * levels
    cnt = here(count)
    lane = lane_ids(*cnt.shape)
    cnt_e = jnp.where(lane == cols - 1, -1.0, jnp.minimum(cnt, turned(cnt, -1)))
    cnt_w = jnp.where(lane == 0, -1.0, jnp.minimum(cnt, turned(cnt, 1)))
    cnt_n = jnp.where(row == size.rows - 1, -1.0, jnp.minimum(cnt, over(count)))
    cnt_s = jnp.where(row == 0, -1.0, jnp.minimum(cnt, under(count)))
    totals = [jnp.zeros(cnt.shape, F32)] * 5
    for k in range(levels):
        level = first_level + k
        wet, wet_e, wet_w, wet_n, wet_s = (
            level < c for c in (cnt, cnt_e, cnt_w, cnt_n, cnt_s)
        )
        u, v, p = here(k), here(levels + k), here(2 * levels + k)
        slow_u, slow_v, push = VISCOSITY * u, VISCOSITY * v, 0.5 * p
        u_less, u_more = slow_u - push, slow_u + push
        gain_e = jnp.where(wet_e, turned(u_less, -1) - u_less, 0.0)
        gain_e = gain_e + jnp.where(wet_w, turned(u_more, 1) - u_more, 0.0)
        gain_n = jnp.where(wet_e, turned(slow_v, -1) - slow_v, 0.0)
        gain_n = gain_n + jnp.where(wet_w, turned(slow_v, 1) - slow_v, 0.0)
        n_u, s_u = over(k) - u, under(k) - u
        n_v, s_v = over(levels + k) - v, under(levels + k) - v
        n_p, s_p = over(2 * levels + k) - p, p - under(2 * levels + k)
        gain_e = gain_e + VISCOSITY * (jnp.where(wet_n, n_u, 0.0) + jnp.where(wet_s, s_u, 0.0))
        gain_n = gain_n + jnp.where(wet_n, VISCOSITY * n_v - 0.5 * n_p, 0.0)
        gain_n = gain_n + jnp.where(wet_s, VISCOSITY * s_v - 0.5 * s_p, 0.0)
        wet_u, wet_v = jnp.where(wet, u, 0.0), jnp.where(wet, v, 0.0)
        tend_e, tend_n = gain_e + cor * wet_v, gain_n - cor * wet_u
        if write is not None:
            write(0, k, wet_u + TIMESTEP * tend_e)
            write(1, k, wet_v + TIMESTEP * tend_n)
        weight = weights[k]
        parts = (weight * tend_e, weight * tend_n, weight * wet_u, weight * wet_v)
        parts += (jnp.where(wet, weight, 0.0),)
        totals = [total + part for total, part in zip(totals, parts)]
    return totals


def edge_kernel(
    size, thick_hbm, east, north, press, surface, land, bottom, coriolis,
    y_first, y_second, weights, thick, levels_of, flat, whole, sems,
):
    levels, rows, cols = size.levels, size.rows, size.cols
    first_level = (lax.axis_index("gz") * levels).astype(F32)
    copies = [pltpu.make_async_copy(thick_hbm, thick, sems.at[0])]
    ends = ((0, REACH), (rows - CHUNK, 4 * REACH))
    for source, target in ends:
        span = pl.ds(source, CHUNK)
        for slot, array in enumerate((east, north, press)):
            at = levels_of.at[pl.ds(slot * levels, levels), pl.ds(target, CHUNK), :]
            copies.append(pltpu.make_async_copy(array.at[:, span, :], at, sems.at[len(copies)]))
    for part, (source, target) in enumerate(ends):
        span = pl.ds(source, CHUNK)
        for index, array in enumerate((land, bottom)):
            at = whole.at[index, pl.ds(part * CHUNK, CHUNK), :]
            copies.append(pltpu.make_async_copy(array.at[span, :], at, sems.at[len(copies)]))
        for index, array in enumerate((surface, coriolis)):
            at = flat.at[index, pl.ds(target, CHUNK), :]
            copies.append(pltpu.make_async_copy(array.at[span, :], at, sems.at[len(copies)]))
    for copy in copies:
        copy.start()
    for copy in copies:
        copy.wait()
    weights[0] = by_level(thick, row_ids(REACH, cols))
    weights[1] = by_level(thick, lane_ids(REACH, cols) % REACH)
    for k in range(levels):
        weights[2 + k] = jnp.full((REACH, cols), thick[k])
    for part, (_, target) in enumerate(ends):
        span = slice(part * CHUNK, part * CHUNK + CHUNK)
        count = whole[0, span, :].astype(F32) * whole[1, span, :].astype(F32)
        levels_of[3 * levels, target : target + CHUNK, :] = count

    starts = (REACH, 4 * REACH + REACH)

    def joined(ref, plane, move=0):
        return jnp.concatenate([ref[plane, at + move : at + move + REACH, :] for at in starts])

    def load(move):
        return lambda plane: joined(levels_of, plane, move)

    like = (CHUNK, cols)
    row = row_ids(*like)
    row = jnp.where(row < REACH, row, row + rows - CHUNK)
    cor = joined(flat, 1)
    fields = core_chunk(
        size, thick, first_level, row, load(0), load(1), load(-1), cor, None
    )
    fields += [joined(flat, 0), load(0)(3 * levels), cor]
    low, high = pack_lines(size, load(0), like)
    fields.append(low + high)
    y_flag, _ = roles("gy")

    def store(index, south, north):
        y_first[index] = either(y_flag, north, south)
        y_second[index] = either(y_flag, south, north)

    for index, value in enumerate(fields):
        store(index, value[:REACH], value[REACH:])
    for slot in range(3):
        planes = slice(slot * levels, (slot + 1) * levels)
        store(
            FIELDS + 1 + slot,
            *(levels_of[planes, at, :] for at in (REACH, 4 * REACH + CHUNK - 1)),
        )


def tile_kernel(
    size, weights, east, north, press, surface, land, bottom, coriolis,
    base, sums, statics, x_first, x_second,
):
    levels, rows, cols = size.levels, size.rows, size.cols
    first_level = (lax.axis_index("gz") * levels).astype(F32)
    span = slice(REACH, REACH + rows)
    statics[0, span, :] = surface[...]
    statics[1, span, :] = land[...].astype(F32) * bottom[...].astype(F32)
    statics[2, span, :] = coriolis[...]
    fields = (east, north, press)
    x_flag, _ = roles("gx")
    like = (CHUNK, cols)
    weight = [jnp.concatenate([weights[2 + k]] * (CHUNK // REACH)) for k in range(levels)]
    for start in range(0, rows, CHUNK):

        def load(move):
            at = start + move

            def value(plane):
                if plane == 3 * levels:
                    return statics[1, REACH + at : REACH + at + CHUNK, :]
                ref, level = fields[plane // levels], plane % levels
                if 0 <= at <= rows - CHUNK:
                    return ref[level, at : at + CHUNK, :]
                return shifted_rows(ref[level, start : start + CHUNK, :], -move)

            return value

        here, place = slice(start, start + CHUNK), slice(start + REACH, start + REACH + CHUNK)

        def write(field, k, value):
            base[field, k, here, :] = value

        totals = core_chunk(
            size, weight, first_level, start + row_ids(*like), load(0), load(1), load(-1),
            statics[2, place, :], write,
        )
        for index, total in enumerate(totals):
            sums[index, place, :] = total
        totals += [statics[index, place, :] for index in range(3)]
        low, high = pack_columns(totals, pack_lines(size, load(0), like), like)
        x_first[place, :] = either(x_flag, high, low)
        x_second[place, :] = either(x_flag, low, high)


def row_kernel(
    size, weights, own_first, own_second, got_first, got_second,
    sums_in, statics_in, x_first_in, x_second_in,
    sums, statics, x_first, x_second, flux,
):
    del sums_in, statics_in, x_first_in, x_second_in
    levels, rows, cols = size.levels, size.rows, size.cols
    first_level = (lax.axis_index("gz") * levels).astype(F32)
    high_first, north_first = roles("gy")
    x_flag, _ = roles("gx")
    top = REACH + rows
    halo = [split(north_first, got_first[i], got_second[i]) for i in range(FIELDS + 4)]
    mine = [split(high_first, own_first[i], own_second[i]) for i in range(FIELDS + 4)]
    row = row_ids(REACH, cols)
    weight, level_of = weights[0], row.astype(F32) + first_level
    end = REACH - 1
    blocks = [
        [pair[part] for pair in pairs[:FIELDS]]
        for pairs, part in ((halo, 0), (mine, 0), (mine, 1), (halo, 1))
    ]
    lines = [
        pairs[FIELDS][part] for pairs, part in ((halo, 0), (mine, 0), (mine, 1), (halo, 1))
    ]
    for side in range(2):
        south = [(halo[i][0], mine[i][1])[side] for i in range(FIELDS + 4)]
        north = [(mine[i][0], halo[i][1])[side] for i in range(FIELDS + 4)]
        counts = jnp.minimum(south[COUNT][end:, :], north[COUNT][:1, :])
        wet = level_of < jnp.broadcast_to(counts, (REACH, cols))
        change_u, change_v, push = (
            jnp.where(wet, north[FIELDS + 1 + slot] - south[FIELDS + 1 + slot], 0.0)
            for slot in range(3)
        )
        change_u, change_v, push = VISCOSITY * change_u, VISCOSITY * change_v, 0.5 * push
        to_north = (-change_u, -change_v - push)
        to_south = (change_u, change_v - push)
        for field in range(2):
            flux[side, field] = (to_north, to_south)[side][field]
            for block, line, value in (
                (2 * side, end, to_south[field]), (2 * side + 1, 0, to_north[field])
            ):
                gain = jnp.sum(weight * value, axis=0, keepdims=True)
                gain = jnp.where(row == line, jnp.broadcast_to(gain, (REACH, cols)), 0.0)
                blocks[block][field] = blocks[block][field] + gain
    slot_of = lane_ids(REACH, cols) // REACH
    for block, start in enumerate((0, REACH, top - REACH, top)):
        place = slice(start, start + REACH)
        for index in range(SUMS):
            sums[index, place, :] = blocks[block][index]
        for index in range(3):
            statics[index, place, :] = blocks[block][SUMS + index]
        low_line = jnp.where((slot_of < 6) & (slot_of % 2 == 0), lines[block], 0.0)
        high_line = jnp.where((slot_of < 6) & (slot_of % 2 == 1), lines[block], 0.0)
        low, high = pack_columns(blocks[block], (low_line, high_line), (REACH, cols))
        x_first[place, :] = either(x_flag, high, low)
        x_second[place, :] = either(x_flag, low, high)


def column_kernel(
    size, weights, own_first, own_second, got_first, got_second, ends, strips, flux,
):
    wide, cols, half = size.wide, size.cols, size.half
    first_level = (lax.axis_index("gz") * size.levels).astype(F32)
    high_first, east_first = roles("gx")
    west, east = split(east_first, got_first[...], got_second[...])
    low, high = split(high_first, own_first[...], own_second[...])
    lane = lane_ids(wide, cols)
    slot_of, place = lane // REACH, lane % REACH
    end = REACH - 1
    change = jnp.where(
        lane < half, turned(low, REACH) - west, turned(turned(east, REACH) - high, half)
    )
    count = 2 * COUNT * REACH + end
    counts = jnp.where(
        lane == count, jnp.minimum(west, turned(low, -1)), jnp.minimum(turned(high, 1), east)
    )
    counts = gathered(counts, jnp.where(lane < half, count, count + 1))
    push = turned(change, -4 * REACH)
    eastward = among(slot_of % FIELDS, (1,))
    wet = (place.astype(F32) + first_level < counts) & among(slot_of % FIELDS, (1, 3))
    change = jnp.where(wet, VISCOSITY * change, 0.0)
    push = jnp.where(wet & eastward, 0.5 * push, 0.0)
    to_east, to_west = -change - push, change - push
    flux[0], flux[1] = to_east, to_west
    weight = jnp.concatenate([weights[1]] * (wide // REACH))
    total = weight * to_east + turned(weight * to_west, 4 * REACH)
    for shift in (1, 2, 4):
        total = total + turned(total, shift)
    outer_west = among(lane, (end, 2 * REACH + end))
    outer_east = among(lane, (REACH, 3 * REACH))
    gain = jnp.where(outer_west, turned(total, -5 * REACH), 0.0)
    gain = gain + jnp.where(outer_east, turned(total, -half - end), 0.0)
    strips[...] = jnp.where(slot_of % 2 == 0, west, east)
    for_west = among(lane, [GAINS + 2 * index * REACH for index in range(2)])
    forces = jnp.where(
        for_west, turned(total, GAINS - REACH - end), turned(total, GAINS - half - 6 * REACH)
    )
    ends[...] = jnp.where(lane < 2 * SUMS * REACH, strips[...] + gain, forces)


def finish_kernel(size, column_flux, row_flux, base_in, base):
    levels, rows, cols = size.levels, size.rows, size.cols
    lane = lane_ids(CHUNK, cols)
    for start in range(0, rows, CHUNK):
        at = slice(start, start + CHUNK)
        wider = slice(start + REACH, start + REACH + CHUNK)
        west, east = column_flux[0, wider, :], column_flux[1, wider, :]
        for field in range(2):
            for k in range(levels):
                source = (2 * field + 1) * REACH + k
                gain = jnp.where(lane == 0, turned(west, -source), 0.0)
                gain = gain + jnp.where(
                    lane == cols - 1, turned(east, size.half - 1 - source), 0.0
                )
                base[field, k, at, :] = base_in[field, k, at, :] + TIMESTEP * gain
    for field in range(2):
        for side, at in enumerate((0, rows - 1)):
            for k in range(levels):
                line = slice(at, at + 1)
                gain = row_flux[side, field, k : k + 1, :]
                base[field, k, line, :] = base[field, k, line, :] + TIMESTEP * gain


H, TE, TN = range(3)
STEP, SLOPE, TURN, PUSH_E, PUSH_N = range(5)


def coefficients(ocean, depth, coriolis, force_east, force_north):
    step = 0.5 * COURANT * ocean
    twice = COURANT * ocean
    return step, step * depth, twice * coriolis, twice * force_east, twice * force_north


def strip_field(size, strips, index):
    lane = lane_ids(*strips.shape)
    moved = turned(strips, (size.slots - 1 - 2 * index) * REACH)
    return jnp.where((lane < REACH) | (lane >= size.cols - REACH), moved, 0.0)


def blend_kernel(size, mine, other, statics, strips, state, fixed, drive):
    here = slice(REACH, REACH + size.wide)
    total = [mine[index] + other[index] for index in range(SUMS)]
    ocean = jnp.where(statics[1] > 0, 1.0, 0.0)
    values = coefficients(ocean, total[4], statics[2], total[0], total[1])
    for index, value in enumerate(values):
        fixed[0, index, here, :] = value
    for index, value in ((TE, total[2]), (TN, total[3]), (H, ocean * statics[0])):
        state[0, index, here, :] = value
    drive[0] = total[2] + TIMESTEP * total[0]
    drive[1] = total[3] + TIMESTEP * total[1]
    drive[2] = total[4] + (1.0 - ocean)
    strips = strips[...]
    ocean = jnp.where(strip_field(size, strips, COUNT) > 0, 1.0, 0.0)
    fixed[1, STEP, here, :] = 0.5 * COURANT * ocean
    fixed[1, TURN, here, :] = COURANT * ocean * strip_field(size, strips, CORIOLIS)
    state[1, H, here, :] = ocean * strip_field(size, strips, SURFACE)


def surface_kernel(
    size, base, statics, mine, other, state_in, fixed_in, drive_in,
    height_out, east_out, north_out, state, fixed, drive,
    result, sems,
):
    del state_in, fixed_in, drive_in
    levels, rows, cols, wide = size.levels, size.rows, size.cols, size.wide
    top = 2 * REACH
    first_level = (lax.axis_index("gz") * levels).astype(F32)

    here, lane = slice(REACH, REACH + wide), lane_ids(wide, cols)
    strips = mine[...] + other[...]
    force_east, force_north, sum_east, sum_north, depth = (
        strip_field(size, strips, index) for index in range(SUMS)
    )
    step = fixed[1, STEP, here, :]
    fixed[1, SLOPE, here, :] = step * depth
    fixed[1, PUSH_E, here, :] = 2.0 * step * force_east
    fixed[1, PUSH_N, here, :] = 2.0 * step * force_north
    state[1, TE, here, :] = sum_east
    state[1, TN, here, :] = sum_north
    for index, push in ((0, PUSH_E), (1, PUSH_N)):
        gain = turned(strips, -GAINS - 2 * index * REACH)
        gain = jnp.where((lane == 0) | (lane == cols - 1), gain, 0.0)
        fixed[0, push, here, :] = (
            fixed[0, push, here, :] + 2.0 * fixed[0, STEP, here, :] * gain
        )
        drive[index] = drive[index] + TIMESTEP * gain
    lane = lane_ids(WAVE, cols)
    at_high, at_low = lane == cols - 1, lane == 0

    def difference_x(field, here):
        inside, outside = state[0, field, here, :], state[1, field, here, :]
        in_e, out_e = turned(inside, -1), turned(outside, -1)
        in_w, out_w = turned(inside, 1), turned(outside, 1)
        return (
            jnp.where(at_high, out_e, in_e) - jnp.where(at_low, out_w, in_w),
            jnp.where(at_high, in_e, out_e) - jnp.where(at_low, in_w, out_w),
        )

    def difference_y(part, field, start):
        above = state[part, field, start + 1 : start + 1 + WAVE, :]
        return above - state[part, field, start - 1 : start - 1 + WAVE, :]

    def height_part(start):
        here = slice(start, start + WAVE)
        across = difference_x(TE, here)
        for part in range(2):
            spread = across[part] + difference_y(part, TN, start)
            state[part, H, here, :] = (
                state[part, H, here, :] - fixed[part, STEP, here, :] * spread
            )

    def transport_part(start):
        here = slice(start, start + WAVE)
        across = difference_x(H, here)
        for part in range(2):
            slope_y = difference_y(part, H, start)
            te, tn = state[part, TE, here, :], state[part, TN, here, :]
            slope, turn, push_e, push_n = (
                fixed[part, index, here, :] for index in (SLOPE, TURN, PUSH_E, PUSH_N)
            )
            state[part, TE, here, :] = te + (turn * tn + push_e - slope * across[part])
            state[part, TN, here, :] = tn + (push_n - turn * te - slope * slope_y)

    for _ in range(SUBSTEPS):
        for part in (height_part, transport_part):
            for start in range(REACH, REACH + wide, WAVE):
                part(start)

    height_copy = pltpu.make_async_copy(
        state.at[0, H, pl.ds(top, rows), :], height_out, sems.at[0]
    )
    height_copy.start()
    inner = slice(top, top + rows)
    floor_depth = drive[2, REACH : REACH + rows, :]
    for index, field in enumerate((TE, TN)):
        gain = state[0, field, inner, :] - drive[index, REACH : REACH + rows, :]
        drive[index, REACH : REACH + rows, :] = gain / floor_depth
    copies = [height_copy]
    for k in range(levels):
        wet = first_level + k < statics[1, REACH : REACH + rows, :]
        for index, out in enumerate((east_out, north_out)):
            change = jnp.where(wet, drive[index, REACH : REACH + rows, :], 0.0)
            result[index, k] = base[index, k] + change
            copy = pltpu.make_async_copy(
                result.at[index, k], out.at[k], sems.at[1 + 2 * k + index]
            )
            copy.start()
            copies.append(copy)
    for copy in copies:
        copy.wait()


VMEM = pl.BlockSpec(memory_space=pltpu.VMEM)
SMEM = pl.BlockSpec(memory_space=pltpu.SMEM)
HBM = pl.BlockSpec(memory_space=pltpu.HBM)


def shaped(*shape):
    return jax.ShapeDtypeStruct(shape, F32)


def call(body, size, ins, outs, shapes, scratch=(), aliases=None, flops=0):
    return pl.pallas_call(
        functools.partial(body, size),
        in_specs=ins,
        out_specs=outs,
        out_shape=shapes,
        scratch_shapes=scratch,
        input_output_aliases=aliases or {},
        compiler_params=pltpu.CompilerParams(vmem_limit_bytes=24 * 1024 * 1024),
        cost_estimate=pl.CostEstimate(flops=flops, bytes_accessed=0, transcendentals=0),
    )


def swapped(axis, first, second):
    pairs = pairing(axis)
    first = lax.ppermute(first, axis, pairs[0])
    second = lax.ppermute(second, axis, pairs[1])
    return first, second


def on_device(
    layer_east, layer_north, layer_press, surface, land_sea, bottom_level, coriolis, level_thick
):
    size = Sizes(*layer_east.shape)
    levels, rows, cols = layer_east.shape
    wide = size.wide
    inputs = [
        pltpu.with_memory_space_constraint(array, pltpu.HBM)
        for array in (
            level_thick, layer_east, layer_north, layer_press,
            surface, land_sea, bottom_level, coriolis,
        )
    ]
    side = shaped(FIELDS + 4, REACH, cols)
    *own_y, weights = call(
        edge_kernel,
        size,
        [HBM] * 8,
        [VMEM] * 3,
        [side, side, shaped(2 + levels, REACH, cols)],
        [
            pltpu.SMEM((levels,), F32),
            pltpu.VMEM((3 * levels + 1, 7 * REACH, cols), F32),
            pltpu.VMEM((2, 7 * REACH, cols), F32),
            pltpu.VMEM((2, 2 * CHUNK, cols), jnp.int32),
            pltpu.SemaphoreType.DMA((15,)),
        ],
    )(*inputs)
    got_y = swapped("gy", *own_y)
    packed = shaped(wide, cols)
    base, sums, statics, x_first, x_second = call(
        tile_kernel,
        size,
        [VMEM] * 8,
        [VMEM] * 5,
        [
            shaped(2, levels, rows, cols),
            shaped(SUMS, wide, cols),
            shaped(3, wide, cols),
            packed,
            packed,
        ],
        flops=10**7,
    )(
        weights, layer_east, layer_north, layer_press,
        surface, land_sea, bottom_level, coriolis,
    )
    sums, statics, x_first, x_second, row_flux = call(
        row_kernel,
        size,
        [VMEM] * 9,
        [VMEM] * 5,
        [
            shaped(SUMS, wide, cols),
            shaped(3, wide, cols),
            packed,
            packed,
            shaped(2, 2, levels, cols),
        ],
        aliases={5: 0, 6: 1, 7: 2, 8: 3},
    )(weights, *own_y, *got_y, sums, statics, x_first, x_second)
    got_x = swapped("gx", x_first, x_second)
    other_sums = lax.ppermute(sums, "gz", pairing("gz")[0])
    scratch = [
        shaped(2, 3, wide + 2 * REACH, cols),
        shaped(2, 5, wide + 2 * REACH, cols),
        shaped(3, wide, cols),
    ]
    ends, strips, column_flux = call(
        column_kernel,
        size,
        [VMEM] * 5,
        [VMEM] * 3,
        [packed, packed, shaped(2, wide, cols)],
    )(weights, x_first, x_second, *got_x)
    other_ends = lax.ppermute(ends, "gz", pairing("gz")[0])
    blended = call(blend_kernel, size, [VMEM] * 4, [VMEM] * 3, scratch, flops=10**6)(
        sums, other_sums, statics, strips
    )
    base = call(
        finish_kernel,
        size,
        [VMEM] * 3,
        [VMEM],
        [shaped(2, levels, rows, cols)],
        aliases={2: 0},
        flops=10**7,
    )(column_flux, row_flux, base)[0]
    layers = shaped(levels, rows, cols)
    height, east_next, north_next, *_ = call(
        surface_kernel,
        size,
        [VMEM] * 7,
        [HBM] * 3 + [VMEM] * 3,
        [shaped(rows, cols), layers, layers, *scratch],
        [
            pltpu.VMEM((2, levels, rows, cols), F32),
            pltpu.SemaphoreType.DMA((1 + 2 * levels,)),
        ],
        aliases={4: 3, 5: 4, 6: 5},
    )(base, statics, ends, other_ends, *blended)
    return (height, east_next, north_next)


def solution(mesh):
    return jax.shard_map(
        on_device,
        mesh=mesh,
        in_specs=(
            P("gz", "gy", "gx"),
            P("gz", "gy", "gx"),
            P("gz", "gy", "gx"),
            P("gy", "gx"),
            P("gy", "gx"),
            P("gy", "gx"),
            P("gy", "gx"),
            P("gz"),
        ),
        out_specs=(P("gy", "gx"), P("gz", "gy", "gx"), P("gz", "gy", "gx")),
        check_vma=False,
    )
```
